32 devices in a mesh: gx: 4 (over y, x), gy: 4 (over z), gz: 2 (over core).
Axes of the slice: x: 2, y: 2, z: 4, core: 2. Of those that a mesh axis runs over, the one named last changes fastest.
Arguments:
- element_load: float32 [36, 36, 18, 128], P('gx', 'gy', 'gz'), may hold values from -90 to 90
- local_matrix: float32 [4, 4, 2, 729, 729], P('gx', 'gy', 'gz'), may hold values from -10 to 61, as said below
- dirichlet_inverse: float32 [4, 4, 2, 343, 343], P('gx', 'gy', 'gz'), as said below
- neumann_inverse: float32 [4, 4, 2, 729, 729], P('gx', 'gy', 'gz'), as said below
- coarse_basis: float32 [4, 4, 2, 20, 729], P('gx', 'gy', 'gz'), as said below
Outputs:
- solution: float32 [36, 36, 18, 128], P('gx', 'gy', 'gz')
- residual: float32 [36, 36, 18, 128], P('gx', 'gy', 'gz')
The draws below stay inside these ranges and needn't reach their ends.
Inputs may be any that keep to these rules, and one draw needn't show every extreme that they name: `local_matrix`: block (a, b, c) is the symmetric positive definite stiffness matrix of subdomain (a, b, c) in the node order of the steps: cellwise conductivities on the couplings of neighbouring nodes plus a lumped reaction term. `dirichlet_inverse`: block (a, b, c) is the inverse, computed in float32, of local_matrix's block restricted to the inner nodes. `neumann_inverse`: block (a, b, c) is the node-by-node block of the inverse, computed in float32, of the saddle-point matrix [[A, Cm^T], [Cm, 0]], with A local_matrix's block and Cm the 20 x 729 primal constraints in the order of the coarse numbering: the value at each of the 8 corners, then the mean over the 7 inner nodes of each of the 12 edges. `coarse_basis`: block (a, b, c) is the constraint-by-node block of that same saddle-point inverse.
All inputs are finite; a program needn't handle non-finite values.
Results may differ from the reference program's by a relative error of at most 0.0014.
Values sent between devices are 32-bit elements; how exact they have to be, the bound alone decides.
No kernel may reach another device: no remote copies, remote signals or barrier semaphores. Data moves between devices by JAX's collectives and lax.ppermute only.
A program may use at most 128 MiB of HBM per device.

```python
import jax
import jax.numpy as jnp
import numpy as np
from jax import lax

CELLS = 8
PRIMAL = 20
RHS = 128
ITERS = 2
N_GX = 4
N_GY = 4
N_GZ = 2


REACTION = 0.004


def conductivity(key):
    shape = (N_GX * N_GY * N_GZ, CELLS, CELLS, CELLS)
    subkey = jax.random.fold_in(key, 7)
    logs = jax.random.uniform(subkey, shape, jnp.float32, np.log(0.3), np.log(3.0))
    return jnp.exp(logs)


def stiffness_of(kappa):
    node_side = CELLS + 1
    node_count = node_side ** 3
    index = jnp.arange(node_count, dtype=jnp.int32).reshape(node_side, node_side, node_side)
    padded = jnp.pad(kappa, 1)
    part_x = padded[1:-1, :, :]
    weight_x = (part_x[:, :-1, :-1] + part_x[:, 1:, :-1] + part_x[:, :-1, 1:] + part_x[:, 1:, 1:]) / 4.0
    part_y = padded[:, 1:-1, :]
    weight_y = (part_y[:-1, :, :-1] + part_y[1:, :, :-1] + part_y[:-1, :, 1:] + part_y[1:, :, 1:]) / 4.0
    part_z = padded[:, :, 1:-1]
    weight_z = (part_z[:-1, :-1, :] + part_z[1:, :-1, :] + part_z[:-1, 1:, :] + part_z[1:, 1:, :]) / 4.0
    pairs = ((weight_x, index[:-1, :, :], index[1:, :, :]), (weight_y, index[:, :-1, :], index[:, 1:, :]), (weight_z, index[:, :, :-1], index[:, :, 1:]))
    matrix = jnp.zeros((node_count, node_count), jnp.float32)
    for weights, lower, upper in pairs:
        weights = weights.reshape(-1)
        lower = lower.reshape(-1)
        upper = upper.reshape(-1)
        matrix = matrix.at[lower, lower].add(weights).at[upper, upper].add(weights)
        matrix = matrix.at[lower, upper].add(-weights).at[upper, lower].add(-weights)
    cell_pad = jnp.pad(jnp.ones((CELLS, CELLS, CELLS), jnp.float32), 1)
    adjacent = jnp.zeros((node_side, node_side, node_side), jnp.float32)
    for shift_x in (0, 1):
        for shift_y in (0, 1):
            for shift_z in (0, 1):
                adjacent = adjacent + cell_pad[shift_x:shift_x + node_side, shift_y:shift_y + node_side, shift_z:shift_z + node_side]
    return matrix + jnp.diag(REACTION * adjacent.reshape(-1) / 8.0)


def constraint_table():
    node_side = CELLS + 1
    node_count = node_side ** 3
    top_index = node_side - 1
    table = np.zeros((20, node_count), np.float32)

    def node_at(first_i, second_j, third_k):
        return (first_i * node_side + second_j) * node_side + third_k
    row = 0
    for sx in (0, 1):
        for sy in (0, 1):
            for sz in (0, 1):
                table[row, node_at(sx * top_index, sy * top_index, sz * top_index)] = 1.0
                row += 1
    for sy in (0, 1):
        for sz in (0, 1):
            for place in range(1, top_index):
                table[row, node_at(place, sy * top_index, sz * top_index)] = 1.0 / (top_index - 1)
            row += 1
    for sx in (0, 1):
        for sz in (0, 1):
            for place in range(1, top_index):
                table[row, node_at(sx * top_index, place, sz * top_index)] = 1.0 / (top_index - 1)
            row += 1
    for sx in (0, 1):
        for sy in (0, 1):
            for place in range(1, top_index):
                table[row, node_at(sx * top_index, sy * top_index, place)] = 1.0 / (top_index - 1)
            row += 1
    return table


def all_stiffness(key):
    return jax.vmap(stiffness_of)(conductivity(key))


def saddle_inverse(matrix):
    table = jnp.asarray(constraint_table())
    zeros_block = jnp.zeros((table.shape[0], table.shape[0]), jnp.float32)
    saddle = jnp.concatenate([jnp.concatenate([matrix, table.T], axis=1), jnp.concatenate([table, zeros_block], axis=1)], axis=0)
    return jnp.linalg.inv(saddle)


def draw_local_matrix(key, part):
    node_count = (CELLS + 1) ** 3
    return all_stiffness(key).reshape(N_GX, N_GY, N_GZ, node_count, node_count)


def draw_dirichlet_inverse(key, part):
    node_side = CELLS + 1
    inner_count = (CELLS - 1) ** 3
    matrices = all_stiffness(key)
    shaped = matrices.reshape(-1, node_side, node_side, node_side, node_side, node_side, node_side)
    inner = shaped[:, 1:-1, 1:-1, 1:-1, 1:-1, 1:-1, 1:-1].reshape(-1, inner_count, inner_count)
    inverse = jnp.linalg.inv(inner)
    inverse = 0.5 * (inverse + jnp.swapaxes(inverse, 1, 2))
    return inverse.reshape(N_GX, N_GY, N_GZ, inner_count, inner_count)


def draw_neumann_inverse(key, part):
    node_count = (CELLS + 1) ** 3
    inverse = jax.vmap(saddle_inverse)(all_stiffness(key))
    top_block = inverse[:, :node_count, :node_count]
    top_block = 0.5 * (top_block + jnp.swapaxes(top_block, 1, 2))
    return top_block.reshape(N_GX, N_GY, N_GZ, node_count, node_count)


def draw_coarse_basis(key, part):
    node_count = (CELLS + 1) ** 3
    inverse = jax.vmap(saddle_inverse)(all_stiffness(key))
    lower_block = inverse[:, node_count:, :node_count]
    upper_block = jnp.swapaxes(inverse[:, :node_count, node_count:], 1, 2)
    basis = 0.5 * (lower_block + upper_block)
    return basis.reshape(N_GX, N_GY, N_GZ, 20, node_count)


def draw_element_load(key, part):
    node_side = CELLS + 1
    devices = N_GX * N_GY * N_GZ
    noise = jax.random.normal(jax.random.fold_in(key, 31), (N_GX, node_side, N_GY, node_side, N_GZ, node_side, RHS), jnp.float32)
    noise = jnp.clip(noise, -4.0, 4.0)
    column_scale = jnp.exp(jax.random.uniform(jax.random.fold_in(key, 37), (RHS,), jnp.float32, np.log(0.3), np.log(3.0)))
    linear = jnp.arange(N_GX, dtype=jnp.float32)[:, None, None, None, None, None, None] * (N_GY * N_GZ) + jnp.arange(N_GY, dtype=jnp.float32)[None, None, :, None, None, None, None] * N_GZ + jnp.arange(N_GZ, dtype=jnp.float32)[None, None, None, None, :, None, None]
    fraction = linear / max(devices - 1, 1)
    values = noise * column_scale * jnp.exp(fraction * np.log(3.0))
    values = jnp.clip(values, -90.0, 90.0)
    return values.reshape(N_GX * node_side, N_GY * node_side, N_GZ * node_side, RHS)


def setup_inputs(seed: int = 0) -> dict:
    key_of = jax.random.split(jax.random.key(seed), 6)
    element_load = draw_element_load(jax.random.fold_in(key_of[5], 71), 0)
    local_matrix = draw_local_matrix(jax.random.fold_in(key_of[5], 71), 0)
    dirichlet_inverse = draw_dirichlet_inverse(jax.random.fold_in(key_of[5], 71), 0)
    neumann_inverse = draw_neumann_inverse(jax.random.fold_in(key_of[5], 71), 0)
    coarse_basis = draw_coarse_basis(jax.random.fold_in(key_of[5], 71), 0)
    return dict(element_load=element_load, local_matrix=local_matrix, dirichlet_inverse=dirichlet_inverse, neumann_inverse=neumann_inverse, coarse_basis=coarse_basis)


def coarse_ids(along_x, along_y, along_z, count_x, count_y, count_z):
    total = count_x * count_y * count_z

    def vertex(shift_x, shift_y, shift_z):
        return ((along_x + shift_x) % count_x * count_y + (along_y + shift_y) % count_y) * count_z + (along_z + shift_z) % count_z
    listed = [vertex(sx, sy, sz) for sx in (0, 1) for sy in (0, 1) for sz in (0, 1)]
    listed += [total + vertex(0, sy, sz) for sy in (0, 1) for sz in (0, 1)]
    listed += [2 * total + vertex(sx, 0, sz) for sx in (0, 1) for sz in (0, 1)]
    listed += [3 * total + vertex(sx, sy, 0) for sx in (0, 1) for sy in (0, 1)]
    return jnp.stack(listed, axis=-1).astype(jnp.int32)

def node_weights(node_side):
    places = jnp.arange(node_side, dtype=jnp.int32)
    on_rim = ((places == 0) | (places == node_side - 1)).astype(jnp.int32)
    rims = on_rim[:, None, None] + on_rim[None, :, None] + on_rim[None, None, :]
    copies = (1.0 + on_rim[:, None, None].astype(jnp.float32)) * (1.0 + on_rim[None, :, None].astype(jnp.float32)) * (1.0 + on_rim[None, None, :].astype(jnp.float32))
    share = (1.0 / copies)[..., None]
    border = jnp.where(rims[..., None] > 0, share, jnp.zeros_like(share))
    return (share, border)

def fold_axis(field, block_axis, node_axis):
    moved = jnp.moveaxis(field, (block_axis, node_axis), (0, 1))
    from_low = jnp.roll(moved[:, -1], 1, axis=0)
    from_high = jnp.roll(moved[:, 0], -1, axis=0)
    moved = moved.at[:, 0].add(from_low)
    moved = moved.at[:, -1].add(from_high)
    return jnp.moveaxis(moved, (0, 1), (block_axis, node_axis))

def assemble(field):
    for block_axis, node_axis in ((0, 3), (1, 4), (2, 5)):
        field = fold_axis(field, block_axis, node_axis)
    return field

def reference(element_load, local_matrix, dirichlet_inverse, neumann_inverse, coarse_basis):
    highest = lax.Precision.HIGHEST
    node_side = CELLS + 1
    node_count = node_side ** 3
    inner_side = node_side - 2
    inner_count = inner_side ** 3
    rhs_count = element_load.shape[-1]
    devices = N_GX * N_GY * N_GZ
    coarse_count = 4 * devices
    cube_shape = (N_GX, N_GY, N_GZ, node_side, node_side, node_side, rhs_count)
    inner_shape = (N_GX, N_GY, N_GZ, inner_side, inner_side, inner_side, rhs_count)

    def to_blocks(field):
        return field.reshape(N_GX, node_side, N_GY, node_side, N_GZ, node_side, rhs_count).transpose(0, 2, 4, 1, 3, 5, 6)

    def from_blocks(field):
        return field.transpose(0, 3, 1, 4, 2, 5, 6).reshape(N_GX * node_side, N_GY * node_side, N_GZ * node_side, rhs_count)
    stiffness = local_matrix.reshape(devices, node_count, node_count)
    stiff_cols = stiffness.reshape(devices, node_count, node_side, node_side, node_side)[:, :, 1:-1, 1:-1, 1:-1].reshape(devices, node_count, inner_count)
    stiff_rows = stiffness.reshape(devices, node_side, node_side, node_side, node_count)[:, 1:-1, 1:-1, 1:-1].reshape(devices, inner_count, node_count)
    interior_inverse = dirichlet_inverse.reshape(devices, inner_count, inner_count)
    neumann = neumann_inverse.reshape(devices, node_count, node_count)
    basis = coarse_basis.reshape(devices, PRIMAL, node_count)
    share, border = node_weights(node_side)
    grid_shape = (N_GX, N_GY, N_GZ)
    along_x = jnp.broadcast_to(jnp.arange(N_GX, dtype=jnp.int32)[:, None, None], grid_shape)
    along_y = jnp.broadcast_to(jnp.arange(N_GY, dtype=jnp.int32)[None, :, None], grid_shape)
    along_z = jnp.broadcast_to(jnp.arange(N_GZ, dtype=jnp.int32)[None, None, :], grid_shape)
    numbers = coarse_ids(along_x, along_y, along_z, N_GX, N_GY, N_GZ).reshape(devices, PRIMAL)
    indicator = (numbers[:, :, None] == jnp.arange(coarse_count, dtype=jnp.int32)[None, None, :]).astype(jnp.float32)

    def product(matrix, flat):
        return jnp.einsum('zmn,znk->zmk', matrix, flat, precision=highest)
    stiff_basis = jnp.einsum('znm,zqm->znq', stiffness, basis, precision=highest)
    coarse_local = jnp.einsum('zpn,znq->zpq', basis, stiff_basis, precision=highest)
    partial_rows = jnp.einsum('zpm,zpq->zmq', indicator, coarse_local, precision=highest)
    coarse_matrix = jnp.einsum('zmq,zqn->mn', partial_rows, indicator, precision=highest)
    factor = jnp.linalg.cholesky(coarse_matrix)

    def dot_all(left, right):
        return jnp.sum(left * right * share, axis=(0, 1, 2, 3, 4, 5))

    def apply_operator(field):
        return assemble(product(stiffness, field.reshape(devices, node_count, rhs_count)).reshape(cube_shape))

    def precondition(current):
        inner_part = current[:, :, :, 1:-1, 1:-1, 1:-1].reshape(devices, inner_count, rhs_count)
        start = product(interior_inverse, inner_part)
        spill = product(stiff_cols, start).reshape(cube_shape)
        first_residual = current - assemble(spill)
        weighted = (border * first_residual).reshape(devices, node_count, rhs_count)
        local_part = product(neumann, weighted)
        primal_load = product(basis, weighted)
        coarse_rhs = jnp.einsum('zpm,zpk->mk', indicator, primal_load, precision=highest)
        coarse_values = jax.scipy.linalg.cho_solve((factor, True), coarse_rhs)
        primal_values = jnp.einsum('zpm,mk->zpk', indicator, coarse_values, precision=highest)
        combined = local_part + jnp.einsum('zpn,zpk->znk', basis, primal_values, precision=highest)
        surface = assemble(border * combined.reshape(cube_shape))
        inner_new = start - product(interior_inverse, product(stiff_rows, surface.reshape(devices, node_count, rhs_count)))
        padded = jnp.pad(inner_new.reshape(inner_shape), ((0, 0), (0, 0), (0, 0), (1, 1), (1, 1), (1, 1), (0, 0)))
        return surface + padded
    right_side = assemble(to_blocks(element_load))
    solution = jnp.zeros(cube_shape, jnp.float32)
    residual = right_side
    precond_now = precondition(residual)
    direction = precond_now
    energy = dot_all(residual, precond_now)
    for iteration in range(ITERS):
        mapped = apply_operator(direction)
        step_size = energy / dot_all(direction, mapped)
        solution = solution + step_size * direction
        residual = residual - step_size * mapped
        if iteration + 1 < ITERS:
            precond_now = precondition(residual)
            energy_next = dot_all(residual, precond_now)
            direction = precond_now + energy_next / energy * direction
            energy = energy_next
    return (from_blocks(solution), from_blocks(residual))
```

```python
import functools

import jax
import jax.numpy as jnp
import numpy as np
from jax import lax
from jax.experimental import pallas as pl
from jax.experimental.pallas import tpu as pltpu
from jax.sharding import PartitionSpec as P

AXES = ("gx", "gy", "gz")
HIGHEST = lax.Precision.HIGHEST
PALLAS = True


def dot(left, right, contract=(1, 0)):
    dims = (((contract[0],), (contract[1],)), ((), ()))
    return lax.dot_general(
        left, right, dims, precision=HIGHEST, preferred_element_type=jnp.float32
    )


def run(function, *operands, flops=10**7):
    if not PALLAS:
        return function(*operands)
    shapes = jax.eval_shape(function, *operands)
    single = not isinstance(shapes, tuple)
    outs = (shapes,) if single else shapes
    count = len(operands)

    def body(*refs):
        results = function(*[ref[...] for ref in refs[:count]])
        results = (results,) if single else results
        for ref, result in zip(refs[count:], results):
            ref[...] = result

    vmem = pl.BlockSpec(memory_space=pltpu.VMEM)
    size = sum(4 * np.prod(x.shape) for x in (*operands, *outs))
    results = pl.pallas_call(
        body,
        out_shape=[jax.ShapeDtypeStruct(x.shape, x.dtype) for x in outs],
        in_specs=[vmem] * count,
        out_specs=[vmem] * len(outs),
        cost_estimate=pl.CostEstimate(
            flops=flops, bytes_accessed=int(size), transcendentals=0
        ),
    )(*operands)
    return results[0] if single else tuple(results)


class Layout:
    def __init__(self, n):
        half = 2 * (n - 1)
        self.n, self.half = n, half
        self.ring_rows = n * 2 * half
        flat = (n - 2) ** 2
        self.flat = -(-flat // 8) * 8
        self.rows = self.ring_rows + 2 * self.flat
        at = lambda i, j, k: (i * n + j) * n + k
        order = []
        for i in range(n):
            for j, k in ((0, 0), (n - 1, n - 1)):
                order += [at(i, j, m) for m in range(n)]
                order += [at(i, m, k) for m in range(1, n - 1)]
        for i in (0, n - 1):
            order += [at(i, j, k) for j in range(1, n - 1) for k in range(1, n - 1)]
            order += [-1] * (self.flat - flat)
        self.order = np.array(order, np.int32)
        inner = range(1, n - 1)
        self.inner = np.array([at(i, j, k) for i in inner for j in inner for k in inner], np.int32)
        share = np.zeros((self.rows, 1), np.float32)
        for row, node in enumerate(order):
            if node >= 0:
                place = (node // (n * n), node // n % n, node % n)
                share[row] = 0.5 ** sum(x in (0, n - 1) for x in place)
        self.share = share

    def split(self, field):
        ring = field[: self.ring_rows].reshape(self.n, 2 * self.half, field.shape[1])
        flat = field[self.ring_rows :].reshape(2, self.flat, field.shape[1])
        return ring, flat

    def join(self, ring, flat):
        width = ring.shape[-1]
        return jnp.concatenate(
            [ring.reshape(self.ring_rows, width), flat.reshape(2 * self.flat, width)], axis=0
        )

    def fold_z(self, ring, below, above):
        n, half = self.n, self.half
        row = lax.broadcasted_iota(jnp.int32, ring.shape, 1)
        swap = lambda x: jnp.concatenate([x[:, half:], x[:, :half]], axis=1)

        def corner(x):
            m = n - 1
            parts = [x[:, s : s + m] for s in (m, 0, half + m, half)]
            return jnp.concatenate(parts, axis=1)

        low_side = (row >= n) & (row < half)
        high_side = row >= half + n
        low_end = (row == 0) | (row == half)
        high_end = (row == n - 1) | (row == half + n - 1)
        zero = jnp.zeros_like(ring)
        if below is above:
            side = jnp.where(low_side | high_side, swap(below), zero)
            return ring + side + jnp.where(low_end | high_end, corner(below), zero)
        ring = ring + jnp.where(low_side, swap(below), zero)
        ring = ring + jnp.where(high_side, swap(above), zero)
        ring = ring + jnp.where(low_end, corner(below), zero)
        return ring + jnp.where(high_end, corner(above), zero)

    def fold_y(self, ring, below, above):
        add = jnp.concatenate([below, above], axis=1)
        row = lax.broadcasted_iota(jnp.int32, ring.shape, 1) % self.half
        return ring + jnp.where(row < self.n, add, jnp.zeros_like(add))

    def fold_x(self, ring, flat, below, above):
        width = 2 * self.half
        first = ring[:1] + below[None, :width]
        last = ring[-1:] + above[None, :width]
        ring = jnp.concatenate([first, ring[1:-1], last], axis=0)
        flat = flat + jnp.stack([below[width:], above[width:]])
        return ring, flat


def shifted(value, axis, step):
    size = lax.axis_size(axis)
    return lax.ppermute(value, axis, [(i, (i + step) % size) for i in range(size)])


def both_ways(low, high, axis):
    return shifted(high, axis, 1), shifted(low, axis, -1)


def gathered(block):
    count = lax.axis_size(AXES)
    spread = jnp.broadcast_to(block[None], (count, *block.shape))
    return lax.all_to_all(spread, AXES, 0, 0, tiled=True)


def cat(parts):
    return parts[0] if len(parts) == 1 else jnp.concatenate(parts, axis=0)


def assemble(layout, fields, finish):
    count = len(fields)
    width = 2 * layout.half
    half = layout.half

    def rings_of(*fields):
        return cat([f[: layout.ring_rows] for f in fields])

    rings = run(rings_of, *fields)
    if lax.axis_size("gz") == 2:
        other = shifted(rings, "gz", 1)
        others = (other,)
    else:
        others = (shifted(rings, "gz", 1), shifted(rings, "gz", -1))

    def after_z(rings, *others):
        shape = (count * layout.n, width, rings.shape[1])
        shaped = [x.reshape(shape) for x in others]
        ring = layout.fold_z(rings.reshape(shape), shaped[0], shaped[-1])
        low = ring[:, :half].reshape(-1, rings.shape[1])
        high = ring[:, half:].reshape(-1, rings.shape[1])
        return ring.reshape(rings.shape), low, high

    rings, low, high = run(after_z, rings, *others)
    below, above = both_ways(low, high, "gy")

    def after_y(rings, below, above, *fields):
        lanes = rings.shape[1]
        shape = (count * layout.n, half, lanes)
        ring = layout.fold_y(
            rings.reshape(count * layout.n, width, lanes), below.reshape(shape), above.reshape(shape)
        )
        ring = ring.reshape(count, layout.n, width, lanes)
        low, high = [], []
        for index, field in enumerate(fields):
            flat = layout.split(field)[1]
            low += [ring[index, 0], flat[0]]
            high += [ring[index, -1], flat[1]]
        return ring.reshape(rings.shape), cat(low), cat(high)

    rings, low, high = run(after_y, rings, below, above, *fields)
    below, above = both_ways(low, high, "gx")
    extra, function = finish

    def after_x(rings, below, above, *rest):
        fields, rest = rest[:count], rest[count:]
        message = width + layout.flat
        done = []
        for index, field in enumerate(fields):
            ring = rings[index * layout.ring_rows : (index + 1) * layout.ring_rows]
            ring = ring.reshape(layout.n, width, rings.shape[1])
            flat = layout.split(field)[1]
            place = slice(index * message, (index + 1) * message)
            done.append(layout.join(*layout.fold_x(ring, flat, below[place], above[place])))
        return function(*done, *rest)

    return run(after_x, rings, below, above, *fields, *extra)


def split3(value):
    high = value.astype(jnp.bfloat16)
    rest = value - high.astype(jnp.float32)
    middle = rest.astype(jnp.bfloat16)
    low = (rest - middle.astype(jnp.float32)).astype(jnp.bfloat16)
    return high, middle, low


def pick_rows(chosen, value):
    total = None
    for part in split3(value):
        term = jnp.dot(chosen, part, preferred_element_type=jnp.float32)
        total = term if total is None else total + term
    return total


def pick_columns(value, chosen):
    total = None
    for part in split3(value):
        term = lax.dot_general(
            part, chosen, (((1,), (1,)), ((), ())), preferred_element_type=jnp.float32
        )
        total = term if total is None else total + term
    return total


def one_hot(places, count):
    columns = lax.broadcasted_iota(jnp.int32, (places.shape[0], count), 1)
    return jnp.where(columns == places, 1.0, 0.0).astype(jnp.bfloat16)


def coarse_table(count_x, count_y, count_z, rows):
    total = count_x * count_y * count_z
    linear = np.arange(total)
    along = (linear // (count_y * count_z), linear // count_z % count_y, linear % count_z)

    def vertex(sx, sy, sz):
        x, y, z = along
        return ((x + sx) % count_x * count_y + (y + sy) % count_y) * count_z + (z + sz) % count_z

    two = (0, 1)
    listed = [vertex(sx, sy, sz) for sx in two for sy in two for sz in two]
    listed += [total + vertex(0, sy, sz) for sy in two for sz in two]
    listed += [2 * total + vertex(sx, 0, sz) for sx in two for sz in two]
    listed += [3 * total + vertex(sx, sy, 0) for sx in two for sy in two]
    table = np.full((total, rows), -1, np.int32)
    table[:, : len(listed)] = np.stack(listed, axis=-1)
    return table


def spd_inverse(matrix):
    count = matrix.shape[0]
    rows = lax.broadcasted_iota(jnp.int32, (count, 1), 0)
    lanes = lax.broadcasted_iota(jnp.int32, (1, count), 1)
    for k in range(count):
        column = matrix[:, k : k + 1]
        pivot = matrix[k : k + 1, k : k + 1]
        row = jnp.where(lanes == k, 1.0, matrix[k : k + 1, :]) / pivot
        kept = jnp.where(lanes == k, 0.0, matrix)
        factor = jnp.where(rows == k, 0.0, column)
        matrix = jnp.where(rows == k, 0.0, kept) - factor * row + jnp.where(rows == k, row, 0.0)
    return matrix


def local(element_load, local_matrix, dirichlet_inverse, neumann_inverse, coarse_basis):
    n = element_load.shape[0]
    lanes = element_load.shape[3]
    node_count = n**3
    layout = Layout(n)
    inner_count = (n - 2) ** 3
    primal = coarse_basis.shape[3]
    stiffness = local_matrix.reshape(node_count, node_count)
    interior_inverse = dirichlet_inverse.reshape(inner_count, inner_count)
    neumann = neumann_inverse.reshape(node_count, node_count)
    basis = coarse_basis.reshape(primal, node_count)
    counts = [lax.axis_size(axis) for axis in AXES]
    chunk = -(-primal // 8) * 8
    table = coarse_table(*counts, chunk)
    coarse_count = 4 * counts[0] * counts[1] * counts[2]
    me = lax.axis_index(AXES)
    own_ids = lax.dynamic_slice_in_dim(jnp.asarray(table), me, 1, axis=0).reshape(chunk, 1)
    all_ids = jnp.asarray(table.reshape(-1, 1))
    order = jnp.asarray(layout.order[:, None])
    inner = jnp.asarray(layout.inner[:, None])
    share = jnp.asarray(layout.share)
    share_row = jnp.asarray(layout.share.reshape(1, -1))
    basis = jnp.pad(basis, ((0, chunk - primal), (0, 0)))

    load = element_load.reshape(node_count, lanes)

    def start(stiffness, interior_inverse, basis, load, order, inner, share_row, own_ids):
        surface = one_hot(order, node_count)
        inside = one_hot(inner, node_count)
        picked = pick_columns(stiffness, surface)
        within = pick_rows(surface, picked)
        coupling = pick_rows(inside, picked)
        load_surface = pick_rows(surface, load)
        load_inside = pick_rows(inside, load)
        begun = dot(interior_inverse, load_inside)
        condensed = load_surface - dot(coupling, begun, (0, 0))
        weighted = pick_columns(basis, surface) * share_row
        own = one_hot(own_ids, coarse_count)
        three = [
            lax.dot_general(
                part, own, (((0,), (0,)), ((), ())), preferred_element_type=jnp.float32
            )
            for part in split3(weighted)
        ]
        spread = three[0] + three[1] + three[2]
        tau = jnp.sum(load_inside * begun, axis=0, keepdims=True)
        coarse_local = dot(dot(basis, stiffness), basis, (1, 1))
        coarse_rows = dot(coarse_local, own.astype(jnp.float32))
        return (
            within, coupling, load_surface, load_inside, begun, condensed, weighted, spread, tau,
            coarse_rows,
        )

    (
        within, coupling, load_surface, load_inside, begun, condensed, weighted, spread, tau,
        coarse_rows,
    ) = run(start, stiffness, interior_inverse, basis, load, order, inner, share_row, own_ids)

    def reorder(neumann, order, share, share_row):
        surface = one_hot(order, node_count)
        return pick_rows(surface, pick_columns(neumann, surface)) * share * share_row

    scaled = run(reorder, neumann, order, share, share_row)

    coarse_all = gathered(coarse_rows).reshape(-1, coarse_count)

    def gather_sum(all_ids, rows):
        indicator = one_hot(all_ids, coarse_count)
        return sum(
            lax.dot_general(
                indicator, part, (((0,), (0,)), ((), ())), preferred_element_type=jnp.float32
            )
            for part in split3(rows)
        )

    def invert(all_ids, rows):
        return spd_inverse(gather_sum(all_ids, rows))

    if coarse_count <= 128:
        coarse_inverse = run(invert, all_ids, coarse_all)
    else:
        factor = jnp.linalg.cholesky(run(gather_sum, all_ids, coarse_all))
        coarse_inverse = jax.scipy.linalg.cho_solve(
            (factor, True), jnp.eye(coarse_count, dtype=jnp.float32)
        )

    def neumann_step(field, scaled, weighted):
        return dot(scaled, field), dot(weighted, field)

    def first_step(field, spread, scaled, weighted):
        return (field, spread, *neumann_step(field, scaled, weighted))

    def add_rows(loads, extra):
        rows = lax.broadcasted_iota(jnp.int32, loads.shape, 0)
        for index, value in enumerate(extra):
            loads = jnp.where(rows == primal + index, value, loads)
        return loads

    def operate(field, within, coupling, interior_inverse):
        extended = dot(interior_inverse, dot(coupling, field))
        image = dot(within, field) - dot(coupling, extended, (0, 0))
        return image, extended

    def coarse_step(all_ids, rows, coarse_inverse, spread):
        return dot(spread, dot(coarse_inverse, gather_sum(all_ids, rows)))

    pieces = [spread[:, s : s + lanes] for s in range(0, coarse_count, lanes)]

    def first(field, *rest):
        pieces, (scaled, weighted) = rest[:-2], rest[-2:]
        return (field, *pieces, *neumann_step(field, scaled, weighted))

    results = assemble(layout, [condensed, *pieces], ((scaled, weighted), first))
    residual, pieces, (mapped, loads) = results[0], results[1:-2], results[-2:]
    spread = jnp.concatenate(pieces, axis=1) if len(pieces) > 1 else pieces[0]

    coarse0 = run(
        coarse_step, all_ids, gathered(loads).reshape(-1, lanes), coarse_inverse, spread
    )

    def apply_first(mapped, coarse, within, coupling, interior_inverse, condensed, tau):
        field = mapped + coarse
        image, extended = operate(field, within, coupling, interior_inverse)
        energy = tau + jnp.sum(condensed * field, axis=0, keepdims=True)
        curvature = tau + jnp.sum(field * image, axis=0, keepdims=True)
        return field, image, extended, jnp.concatenate([energy, curvature], axis=0)

    field0, image0, extended0, sums0 = assemble(
        layout,
        [mapped],
        ((coarse0, within, coupling, interior_inverse, condensed, tau), apply_first),
    )

    def second(image, load_surface, scaled, weighted, sums):
        mapped, loads = neumann_step(image, scaled, weighted)
        return image, load_surface, mapped, add_rows(loads, [sums[:1], sums[1:2]])

    image0_sum, load_sum, mapped, loads = assemble(
        layout, [image0, load_surface], ((scaled, weighted, sums0), second)
    )
    rows = gathered(loads)
    coarse1 = run(coarse_step, all_ids, rows.reshape(-1, lanes), coarse_inverse, spread)

    def scalars(rows):
        return jnp.sum(rows, axis=0)

    totals0 = run(scalars, rows)[primal : primal + 2]

    def apply_second(
        mapped, coarse, within, coupling, interior_inverse, condensed, tau, field0, image0, totals
    ):
        field = mapped + coarse
        image, extended = operate(field, within, coupling, interior_inverse)
        step = totals[:1] / totals[1:2]
        rest = 1.0 - step
        direction = field0 - step * field
        direction_image = image0 - step * image
        energy = rest * rest * tau + jnp.sum(
            (condensed - step * image0) * direction, axis=0, keepdims=True
        )
        curvature = rest * rest * tau + jnp.sum(
            direction * direction_image, axis=0, keepdims=True
        )
        cross = rest * tau + jnp.sum(direction * image0, axis=0, keepdims=True)
        fill = jnp.zeros((5, tau.shape[1]), jnp.float32)
        return field, image, extended, jnp.concatenate([energy, curvature, cross, fill], axis=0)

    field1, image1, extended1, sums1 = assemble(
        layout,
        [mapped],
        (
            (coarse1, within, coupling, interior_inverse, condensed, tau, field0, image0, totals0),
            apply_second,
        ),
    )
    rows1 = gathered(sums1)

    def finish(
        image1, image0, residual, load_sum, field0, field1, extended0, extended1, begun,
        load_inside, totals, rows,
    ):
        energy, curvature = totals[:1], totals[1:2]
        sums = jnp.sum(rows, axis=0)
        step = energy / curvature
        energy_next, curvature_next, cross = sums[:1], sums[1:2], sums[2:3]
        ratio = energy_next / energy
        curvature_next = curvature_next + 2.0 * ratio * cross + ratio * ratio * curvature
        step_next = energy_next / curvature_next
        first = step + step_next * (1.0 + ratio)
        second = -step_next * step
        solution_surface = first * field0 + second * field1
        solution_inside = (first + second) * begun - (first * extended0 + second * extended1)
        spill = load_sum - residual
        residual_surface = load_sum - first * (image0 + spill) - second * (image1 + spill)
        residual_inside = (1.0 - first - second) * load_inside
        return solution_surface, solution_inside, residual_surface, residual_inside

    out = assemble(
        layout,
        [image1],
        (
            (
                image0_sum, residual, load_sum, field0, field1, extended0, extended1, begun,
                load_inside, totals0, rows1,
            ),
            finish,
        ),
    )
    place = np.zeros(node_count, np.int32)
    for row, node in enumerate(layout.order):
        if node >= 0:
            place[node] = row
    place[layout.inner] = layout.rows + np.arange(inner_count)
    place = jnp.asarray(place[:, None])
    total_rows = layout.rows + inner_count

    def natural(surface, inside, place):
        chosen = one_hot(place, total_rows)
        return pick_rows(chosen, jnp.concatenate([surface, inside], axis=0))

    shape = element_load.shape
    return (
        run(natural, out[0], out[1], place).reshape(shape),
        run(natural, out[2], out[3], place).reshape(shape),
    )


def solution(mesh):
    in_specs = (
        P("gx", "gy", "gz", None),
        P("gx", "gy", "gz", None, None),
        P("gx", "gy", "gz", None, None),
        P("gx", "gy", "gz", None, None),
        P("gx", "gy", "gz", None, None),
    )
    out_specs = (P("gx", "gy", "gz", None), P("gx", "gy", "gz", None))
    return jax.shard_map(local, mesh=mesh, in_specs=in_specs, out_specs=out_specs, check_vma=False)
```

```python
import jax
import jax.numpy as jnp
import numpy as np
from jax import lax
from jax.experimental import pallas as pl
from jax.experimental.pallas import tpu as pltpu
from jax.sharding import PartitionSpec as P

AXES = ("gx", "gy", "gz")
HIGHEST = lax.Precision.HIGHEST
PALLAS = True
LIMIT = 24 * 2**20
VMEM = pltpu.VMEM
PIECES = 4
FILL = 10**8


def dot(left, right, contract=(1, 0)):
    dims = (((contract[0],), (contract[1],)), ((), ()))
    return lax.dot_general(
        left, right, dims, precision=HIGHEST, preferred_element_type=jnp.float32
    )


def whole(count):
    return [pl.BlockSpec(memory_space=VMEM)] * count


def call(body, operands, outs, scratch=(), in_hbm=(), flops=10**6):
    places = whole(len(operands))
    for index in in_hbm:
        places[index] = pl.BlockSpec(memory_space=pl.ANY)
    size = sum(4 * np.prod(x.shape) for x in (*operands, *outs))
    return pl.pallas_call(
        body,
        out_shape=[jax.ShapeDtypeStruct(x.shape, x.dtype) for x in outs],
        in_specs=places,
        out_specs=whole(len(outs)),
        scratch_shapes=scratch,
        compiler_params=pltpu.CompilerParams(vmem_limit_bytes=LIMIT),
        cost_estimate=pl.CostEstimate(flops=flops, bytes_accessed=int(size), transcendentals=0),
    )(*operands)


def run(function, *operands, flops=10**6):
    if not PALLAS:
        return function(*operands)
    shapes = jax.eval_shape(function, *operands)
    single = not isinstance(shapes, tuple)
    outs = (shapes,) if single else shapes
    count = len(operands)

    def body(*refs):
        results = function(*[ref[...] for ref in refs[:count]])
        results = (results,) if single else results
        for ref, result in zip(refs[count:], results):
            ref[...] = result

    results = call(body, operands, outs, flops=flops)
    return results[0] if single else tuple(results)


def floats(*shape):
    return jax.ShapeDtypeStruct(shape, jnp.float32)


class Layout:
    def __init__(self, n):
        m = n - 1
        self.n, self.m = n, m
        self.block = n * m
        self.ring_rows = 4 * self.block
        flat = (n - 2) ** 2
        self.flat = -(-flat // 8) * 8
        self.rows = self.ring_rows + 2 * self.flat
        self.y_rows = self.block + -(-n // 8) * 8
        self.x_rows = 4 * m + self.flat
        at = lambda i, j, k: (i * n + j) * n + k
        inner = range(1, m)
        order = [at(i, j, k) for j in (0, m) for i in range(n) for k in range(m)]
        for j, k in ((0, 0), (m, m)):
            for i in range(n):
                order += [at(i, x, k) for x in inner] + [at(i, j, m)]
        for i in (0, m):
            order += [at(i, j, k) for j in inner for k in inner]
            order += [-1] * (self.flat - flat)
        self.order = np.array(order, np.int32)
        self.inner = np.array([at(i, j, k) for i in inner for j in inner for k in inner], np.int32)
        share = np.zeros((self.rows, 1), np.float32)
        for row, node in enumerate(order):
            if node >= 0:
                place = (node // (n * n), node // n % n, node % n)
                share[row] = 0.5 ** sum(x in (0, m) for x in place)
        self.share = share

    def blocks(self, ring):
        return [ring[s * self.block : (s + 1) * self.block] for s in range(4)]

    def row_in_tile(self, block):
        return lax.broadcasted_iota(jnp.int32, block.shape, 0) % self.m

    def fold_z(self, ring, below, above):
        first, last, low, high = self.blocks(ring)
        below, above = self.blocks(below), self.blocks(above)
        row = self.row_in_tile(first)
        start, end = row == 0, row == self.m - 1
        back = lambda x: roll_rows(x, x.shape[0] - (self.m - 1))
        ahead = lambda x: roll_rows(x, self.m - 1)
        zero = jnp.zeros_like(first)
        first = first + jnp.where(start, back(below[2]), zero)
        last = last + jnp.where(start, back(below[3]), zero)
        low = low + jnp.where(end, ahead(above[0]), below[3])
        high = high + jnp.where(end, ahead(above[1]), above[2])
        return jnp.concatenate([first, last, low, high], axis=0)

    def side(self, block, corners):
        lanes = block.shape[1]
        rows = corners.reshape(self.n, self.m, lanes)[:, self.m - 1, :]
        fill = jnp.zeros((self.y_rows - self.block - self.n, lanes), block.dtype)
        return jnp.concatenate([block, rows, fill], axis=0)

    def sides_y(self, ring):
        first, last, low, high = self.blocks(ring)
        return self.side(first, low), self.side(last, high)

    def fold_y(self, ring, below, above):
        first, last, low, high = self.blocks(ring)
        lanes = ring.shape[1]
        end = self.row_in_tile(first) == self.m - 1

        def ends(message):
            rows = message[self.block : self.block + self.n].reshape(self.n, 1, lanes)
            wide = jnp.broadcast_to(rows, (self.n, self.m, lanes)).reshape(self.block, lanes)
            return jnp.where(end, wide, jnp.zeros_like(wide))

        first = first + below[: self.block]
        low = low + ends(below)
        last = last + above[: self.block]
        high = high + ends(above)
        return jnp.concatenate([first, last, low, high], axis=0)

    def sides_x(self, ring, flat):
        m, block = self.m, self.block
        low = [ring[s * block : s * block + m] for s in range(4)] + [flat[: self.flat]]
        high = [ring[(s + 1) * block - m : (s + 1) * block] for s in range(4)] + [flat[self.flat :]]
        return jnp.concatenate(low, axis=0), jnp.concatenate(high, axis=0)

    def fold_x(self, ring, flat, below, above):
        m, block = self.m, self.block
        parts = []
        for s in range(4):
            parts += [
                ring[s * block : s * block + m] + below[s * m : (s + 1) * m],
                ring[s * block + m : (s + 1) * block - m],
                ring[(s + 1) * block - m : (s + 1) * block] + above[s * m : (s + 1) * m],
            ]
        parts += [flat[: self.flat] + below[4 * m :], flat[self.flat :] + above[4 * m :]]
        return jnp.concatenate(parts, axis=0)


def roll_rows(value, shift):
    if PALLAS:
        return pltpu.roll(value, shift, 0)
    return jnp.roll(value, shift, axis=0)


def shifted(value, axis, step):
    size = lax.axis_size(axis)
    return lax.ppermute(value, axis, [(i, (i + step) % size) for i in range(size)])


def both_ways(low, high, axis):
    return shifted(high, axis, 1), shifted(low, axis, -1)


def cat(parts):
    return parts[0] if len(parts) == 1 else jnp.concatenate(parts, axis=0)


def assemble(layout, fields, extra, function, flops=10**6):
    count = len(fields)
    rings, rows = layout.ring_rows, layout.rows

    sent = fields if count == 1 else [cat([f[:rings] for f in fields])]
    message = sent[0][:rings] if count == 1 else sent[0]
    if lax.axis_size("gz") == 2:
        others = (shifted(message, "gz", 1),)
    else:
        others = (shifted(message, "gz", 1), shifted(message, "gz", -1))

    def after_z(*values):
        fields, others = values[:count], values[count:]
        done, low, high = [], [], []
        for index, field in enumerate(fields):
            place = slice(index * rings, (index + 1) * rings)
            ring = layout.fold_z(field[:rings], others[0][place], others[-1][place])
            sides = layout.sides_y(ring)
            done.append(ring)
            low.append(sides[0])
            high.append(sides[1])
        return cat(done), cat(low), cat(high)

    ring, low, high = run(after_z, *fields, *others)
    below, above = both_ways(low, high, "gy")

    def after_y(ring, below, above, *fields):
        done, low, high = [], [], []
        for index, field in enumerate(fields):
            place = slice(index * layout.y_rows, (index + 1) * layout.y_rows)
            one = ring[index * rings : (index + 1) * rings]
            one = layout.fold_y(one, below[place], above[place])
            sides = layout.sides_x(one, field[rings:])
            done.append(one)
            low.append(sides[0])
            high.append(sides[1])
        return cat(done), cat(low), cat(high)

    ring, low, high = run(after_y, ring, below, above, *fields)
    below, above = both_ways(low, high, "gx")

    def after_x(ring, below, above, *rest):
        fields, rest = rest[:count], rest[count:]
        done = []
        for index, field in enumerate(fields):
            place = slice(index * layout.x_rows, (index + 1) * layout.x_rows)
            one = ring[index * rings : (index + 1) * rings]
            done.append(layout.fold_x(one, field[rings:], below[place], above[place]))
        return function(*done, *rest)

    return run(after_x, ring, below, above, *fields, *extra, flops=flops)


def parts_of(value):
    high = value.astype(jnp.bfloat16)
    rest = value - high.astype(jnp.float32)
    middle = rest.astype(jnp.bfloat16)
    low = (rest - middle.astype(jnp.float32)).astype(jnp.bfloat16)
    return high, middle, low


def pick(left, right, contract=(1, 0)):
    dims = (((contract[0],), (contract[1],)), ((), ()))
    if left.dtype == jnp.bfloat16:
        pairs = [(left, part) for part in parts_of(right)]
    else:
        pairs = [(part, right) for part in parts_of(left)]
    terms = [lax.dot_general(a, b, dims, preferred_element_type=jnp.float32) for a, b in pairs]
    return terms[0] + terms[1] + terms[2]


def one_hot_rows(column, count):
    lanes = lax.broadcasted_iota(jnp.int32, (column.shape[0], count), 1).astype(jnp.float32)
    return jnp.where(lanes == column, 1.0, 0.0).astype(jnp.bfloat16)


def one_hot_columns(row, count):
    places = lax.broadcasted_iota(jnp.int32, (count, row.shape[1]), 0).astype(jnp.float32)
    return jnp.where(places == row, 1.0, 0.0).astype(jnp.bfloat16)


def as_column(row):
    return jnp.broadcast_to(row, (8, row.shape[1])).T[:, :1]


def coarse_table(count_x, count_y, count_z, rows):
    total = count_x * count_y * count_z
    linear = np.arange(total)
    along = (linear // (count_y * count_z), linear // count_z % count_y, linear % count_z)

    def vertex(sx, sy, sz):
        x, y, z = along
        return ((x + sx) % count_x * count_y + (y + sy) % count_y) * count_z + (z + sz) % count_z

    two = (0, 1)
    listed = [vertex(sx, sy, sz) for sx in two for sy in two for sz in two]
    listed += [total + vertex(0, sy, sz) for sy in two for sz in two]
    listed += [2 * total + vertex(sx, 0, sz) for sx in two for sz in two]
    listed += [3 * total + vertex(sx, sy, 0) for sx in two for sy in two]
    table = np.full((total, rows), -1, np.float32)
    table[:, : len(listed)] = np.stack(listed, axis=-1)
    return table


def eliminate(matrix, pivots):
    count = matrix.shape[0]
    rows = lax.broadcasted_iota(jnp.int32, (count, 1), 0)
    lanes = lax.broadcasted_iota(jnp.int32, (1, count), 1)
    for k in pivots:
        column = matrix[:, k : k + 1]
        pivot = matrix[k : k + 1, k : k + 1]
        row = jnp.where(lanes == k, 1.0, matrix[k : k + 1, :]) / pivot
        kept = jnp.where(lanes == k, 0.0, matrix)
        factor = jnp.where(rows == k, -1.0, column)
        matrix = jnp.where(rows == k, 0.0, kept) - factor * row
    return matrix


def local(element_load, local_matrix, dirichlet_inverse, neumann_inverse, coarse_basis):
    n = element_load.shape[0]
    lanes = element_load.shape[3]
    nodes = n**3
    layout = Layout(n)
    inside = (n - 2) ** 3
    primal = coarse_basis.shape[3]
    counts = [lax.axis_size(axis) for axis in AXES]
    devices = counts[0] * counts[1] * counts[2]
    coarse = 4 * devices
    chunk = -(-primal // 8) * 8
    rows = layout.rows
    table = coarse_table(*counts, chunk)
    own_table = jnp.asarray(np.pad(table, ((0, 0), (0, 128 - chunk)), constant_values=-1))
    all_ids = jnp.asarray(table.reshape(1, -1))
    places = np.stack([layout.order.astype(np.float32), layout.share[:, 0]])
    places = jnp.asarray(np.pad(places, ((0, 6), (0, 0))))
    pairs = [(i, j) for i in range(n) for j in range(n)]
    inner_pairs = [(i, j) for i in range(1, n - 1) for j in range(1, n - 1)]
    deep = n - 2

    def spread_out(block):
        return jnp.broadcast_to(block[None], (devices, *block.shape))

    def start(
        load_in, matrix_in, inverse_in, neumann_in, basis_in, places, own_table,
        condensed, spread, load_surface, load_inside, begun, tau, weighted, coarse_rows,
        matrix, inverse, neumann, load, natural, begun_natural, sems,
    ):
        moves = [
            pltpu.make_async_copy(source, target, sems.at[index])
            for index, (source, target) in enumerate(
                (
                    (load_in, load),
                    (inverse_in.at[0, 0, 0], inverse),
                    (matrix_in.at[0, 0, 0], matrix),
                    (neumann_in.at[0, 0, 0], neumann),
                )
            )
        ]
        for move in moves:
            move.start()
        order = places[0:1, :]
        surface = one_hot_rows(as_column(order), nodes)
        across = one_hot_columns(order, nodes)
        moves[0].wait()
        for i, j in pairs:
            natural[pl.ds((i * n + j) * n, n), :] = load[i, j]
        for index, (i, j) in enumerate(inner_pairs):
            load_inside[pl.ds(index * deep, deep), :] = load[i, j, pl.ds(1, deep), :]
        moves[1].wait()
        begun[...] = dot(inverse[...], load_inside[...])
        tau[...] = jnp.sum(load_inside[...] * begun[...], axis=0, keepdims=True)
        begun_natural[...] = jnp.zeros_like(begun_natural)
        for index, (i, j) in enumerate(inner_pairs):
            begun_natural[pl.ds((i * n + j) * n + 1, deep), :] = begun[pl.ds(index * deep, deep), :]
        basis = jnp.concatenate(
            [basis_in[0, 0, 0], jnp.zeros((chunk - primal, nodes), jnp.float32)], axis=0
        )
        weighted[...] = pick(basis, across) * places[1:2, :]
        own = one_hot_rows(as_column(own_table[pl.ds(lax.axis_index(AXES), 1), :])[:chunk], coarse)
        spread[...] = pick(weighted[...], own, (0, 0))
        wide = jnp.concatenate([basis, jnp.zeros((128 - chunk, nodes), jnp.float32)], axis=0).T
        moves[2].wait()
        images = dot(matrix[...], jnp.concatenate([begun_natural[...], wide], axis=1))
        both = jnp.concatenate([natural[...], natural[...] - images[:, :lanes]], axis=1)
        both = pick(surface, both)
        load_surface[...] = both[:, :lanes]
        condensed[...] = both[:, lanes:]
        coarse_local = dot(basis, images[:, lanes:])
        coarse_rows[...] = spread_out(pick(coarse_local[:, :chunk], own))
        moves[3].wait()

    (
        condensed, spread, load_surface, load_inside, begun, tau, weighted, coarse_rows,
        matrix, inverse, neumann,
    ) = call(
        start,
        (element_load, local_matrix, dirichlet_inverse, neumann_inverse, coarse_basis, places, own_table),
        (
            floats(rows, lanes), floats(rows, coarse), floats(rows, lanes), floats(inside, lanes),
            floats(inside, lanes), floats(1, lanes), floats(chunk, rows),
            floats(devices, chunk, coarse), floats(nodes, nodes), floats(inside, inside),
            floats(nodes, nodes),
        ),
        scratch=[
            VMEM((n, n, n, lanes), jnp.float32), VMEM((nodes, lanes), jnp.float32),
            VMEM((nodes, lanes), jnp.float32), pltpu.SemaphoreType.DMA((4,)),
        ],
        in_hbm=(0, 1, 2, 3),
    )

    coarse_all = lax.all_to_all(coarse_rows, AXES, 0, 0, tiled=True).reshape(-1, coarse)

    def reorder(neumann, places):
        order, share = places[0:1, :], places[1:2, :]
        across = one_hot_columns(order, nodes)
        surface = one_hot_rows(as_column(order), nodes)
        return pick(surface, pick(neumann, across)) * as_column(share) * share

    scaled = run(reorder, neumann, places, flops=FILL)

    def condense(matrix, inverse, places):
        order = places[0:1, :]
        picked = pick(matrix, one_hot_columns(order, nodes))
        surface = one_hot_rows(as_column(order), nodes)
        within = pick(surface, picked)
        coupling = jnp.concatenate(
            [picked[(i * n + j) * n + 1 : (i * n + j) * n + 1 + deep] for i, j in inner_pairs], axis=0
        )
        return within - dot(coupling, dot(inverse, coupling), (0, 0)), coupling

    schur, coupling = run(condense, matrix, inverse, places, flops=FILL)

    def gather_sum(all_ids, rows):
        return pick(one_hot_columns(all_ids, coarse), rows)

    if coarse <= 128:
        step = coarse // PIECES

        def first_piece(all_ids, rows):
            return eliminate(gather_sum(all_ids, rows), range(step))

        coarse_inverse = run(first_piece, all_ids, coarse_all, flops=FILL)
        for piece in range(1, PIECES):

            def next_piece(matrix, piece=piece):
                return eliminate(matrix, range(piece * step, (piece + 1) * step))

            coarse_inverse = run(next_piece, coarse_inverse, flops=FILL)
    else:
        factor = jnp.linalg.cholesky(run(gather_sum, all_ids, coarse_all))
        coarse_inverse = jax.scipy.linalg.cho_solve(
            (factor, True), jnp.eye(coarse, dtype=jnp.float32)
        )

    def neumann_step(field, scaled, weighted):
        return dot(scaled, field), dot(weighted, field)

    def add_rows(loads, extra):
        place = lax.broadcasted_iota(jnp.int32, loads.shape, 0)
        for index in range(extra.shape[0]):
            loads = jnp.where(place == primal + index, extra[index : index + 1], loads)
        return loads

    def coarse_step(all_ids, rows, coarse_inverse, spread):
        return dot(spread, dot(coarse_inverse, gather_sum(all_ids, rows)))

    pieces = [spread[:, s : s + lanes] for s in range(0, coarse, lanes)]

    def first(field, *rest):
        pieces, (scaled, weighted) = rest[:-2], rest[-2:]
        mapped, loads = neumann_step(field, scaled, weighted)
        return (field, *pieces, mapped, spread_out(loads))

    results = assemble(layout, [condensed, *pieces], (scaled, weighted), first)
    residual, pieces, (mapped, loads) = results[0], results[1:-2], results[-2:]
    spread = jnp.concatenate(pieces, axis=1) if len(pieces) > 1 else pieces[0]

    gathered = lax.all_to_all(loads, AXES, 0, 0, tiled=True)
    coarse0 = run(coarse_step, all_ids, gathered.reshape(-1, lanes), coarse_inverse, spread)

    def apply_first(mapped, coarse, schur, condensed, tau):
        field = mapped + coarse
        image = dot(schur, field)
        energy = tau + jnp.sum(condensed * field, axis=0, keepdims=True)
        curvature = tau + jnp.sum(field * image, axis=0, keepdims=True)
        return field, image, jnp.concatenate([energy, curvature], axis=0)

    field0, image0, sums0 = assemble(
        layout, [mapped], (coarse0, schur, condensed, tau), apply_first
    )

    def second(image, load_surface, scaled, weighted, sums):
        mapped, loads = neumann_step(image, scaled, weighted)
        return image, load_surface, mapped, spread_out(add_rows(loads, sums))

    image0_sum, load_sum, mapped, loads = assemble(
        layout, [image0, load_surface], (scaled, weighted, sums0), second
    )
    gathered = lax.all_to_all(loads, AXES, 0, 0, tiled=True)

    def coarse_and_totals(all_ids, rows, coarse_inverse, spread):
        flat = rows.reshape(-1, lanes)
        totals = jnp.sum(rows, axis=0)[primal : primal + 2]
        return coarse_step(all_ids, flat, coarse_inverse, spread), totals

    coarse1, totals0 = run(coarse_and_totals, all_ids, gathered, coarse_inverse, spread)

    def apply_second(mapped, coarse, schur, condensed, tau, field0, image0, totals):
        field = mapped + coarse
        image = dot(schur, field)
        step = totals[:1] / totals[1:2]
        rest = 1.0 - step
        direction = field0 - step * field
        direction_image = image0 - step * image
        energy = rest * rest * tau + jnp.sum(
            (condensed - step * image0) * direction, axis=0, keepdims=True
        )
        curvature = rest * rest * tau + jnp.sum(
            direction * direction_image, axis=0, keepdims=True
        )
        cross = rest * tau + jnp.sum(direction * image0, axis=0, keepdims=True)
        fill = jnp.zeros((5, lanes), jnp.float32)
        sums = jnp.concatenate([energy, curvature, cross, fill], axis=0)
        return field, image, spread_out(sums)

    field1, image1, sums1 = assemble(
        layout, [mapped], (coarse1, schur, condensed, tau, field0, image0, totals0), apply_second
    )
    rows1 = lax.all_to_all(sums1, AXES, 0, 0, tiled=True)

    def weigh(totals, rows, begun, coupling, inverse, field0, field1):
        energy, curvature = totals[:1], totals[1:2]
        sums = jnp.sum(rows, axis=0)
        step = energy / curvature
        energy_next, curvature_next, cross = sums[:1], sums[1:2], sums[2:3]
        ratio = energy_next / energy
        curvature_next = curvature_next + 2.0 * ratio * cross + ratio * ratio * curvature
        step_next = energy_next / curvature_next
        first = step + step_next * (1.0 + ratio)
        second = -step_next * step
        surface = first * field0 + second * field1
        deep = (first + second) * begun - dot(inverse, dot(coupling, surface))
        return surface, deep, jnp.concatenate([first, second], axis=0)

    solution_surface, solution_inside, weights = run(
        weigh, totals0, rows1, begun, coupling, inverse, field0, field1, flops=FILL
    )

    def leftover(image1, image0, residual, load_sum, load_inside, weights):
        first, second = weights[:1], weights[1:2]
        spill = load_sum - residual
        surface = load_sum - first * (image0 + spill) - second * (image1 + spill)
        return surface, (1.0 - first - second) * load_inside

    residual_surface, residual_inside = assemble(
        layout, [image1], (image0_sum, residual, load_sum, load_inside, weights), leftover
    )

    def place(solution_surface, solution_inside, residual_surface, residual_inside, one, two):
        m, block = n - 1, layout.block
        for surface, deep_rows, out in (
            (solution_surface, solution_inside, one), (residual_surface, residual_inside, two)
        ):
            for i in range(n):
                for s, j in ((0, 0), (1, m)):
                    out[i, j, pl.ds(0, m), :] = surface[pl.ds(s * block + i * m, m), :]
                    out[i, j, pl.ds(m, 1), :] = surface[pl.ds((s + 2) * block + i * m + m - 1, 1), :]
                for j in range(1, m):
                    for s, k in ((2, 0), (3, m)):
                        out[i, j, pl.ds(k, 1), :] = surface[pl.ds(s * block + i * m + j - 1, 1), :]
                    if i in (0, m):
                        at = layout.ring_rows + (layout.flat if i else 0) + (j - 1) * deep
                        out[i, j, pl.ds(1, deep), :] = surface[pl.ds(at, deep), :]
                    else:
                        at = ((i - 1) * deep + j - 1) * deep
                        out[i, j, pl.ds(1, deep), :] = deep_rows[pl.ds(at, deep), :]

    shape = floats(*element_load.shape)
    out = call(
        place, (solution_surface, solution_inside, residual_surface, residual_inside), (shape, shape)
    )
    return out[0], out[1]


def solution(mesh):
    in_specs = (
        P("gx", "gy", "gz", None),
        P("gx", "gy", "gz", None, None),
        P("gx", "gy", "gz", None, None),
        P("gx", "gy", "gz", None, None),
        P("gx", "gy", "gz", None, None),
    )
    out_specs = (P("gx", "gy", "gz", None), P("gx", "gy", "gz", None))
    return jax.shard_map(local, mesh=mesh, in_specs=in_specs, out_specs=out_specs, check_vma=False)
```

```python
import jax
import jax.numpy as jnp
import numpy as np
from jax import lax
from jax.experimental import pallas as pl
from jax.experimental.pallas import tpu as pltpu
from jax.sharding import PartitionSpec as P

AXES = ("gx", "gy", "gz")
HIGHEST = lax.Precision.HIGHEST
PALLAS = True
LIMIT = 24 * 2**20
VMEM = pltpu.VMEM
PIECES = 4
PLAIN = 8
FILL = 10**8


def dot(left, right, contract=(1, 0)):
    dims = (((contract[0],), (contract[1],)), ((), ()))
    return lax.dot_general(
        left, right, dims, precision=HIGHEST, preferred_element_type=jnp.float32
    )


def whole(count):
    return [pl.BlockSpec(memory_space=VMEM)] * count


def call(body, operands, outs, scratch=(), in_hbm=(), flops=10**6, aliases=None):
    places = whole(len(operands))
    for index in in_hbm:
        places[index] = pl.BlockSpec(memory_space=pl.ANY)
    size = sum(4 * np.prod(x.shape) for x in (*operands, *outs))
    return pl.pallas_call(
        body,
        out_shape=[jax.ShapeDtypeStruct(x.shape, x.dtype) for x in outs],
        in_specs=places,
        out_specs=whole(len(outs)),
        scratch_shapes=scratch,
        input_output_aliases=aliases or {},
        compiler_params=pltpu.CompilerParams(vmem_limit_bytes=LIMIT),
        cost_estimate=pl.CostEstimate(flops=flops, bytes_accessed=int(size), transcendentals=0),
    )(*operands)


def run(function, *operands, flops=10**6, after=(), keep=None, use=(), store=()):
    arrays = {} if keep is None else keep.arrays
    names = list(arrays)
    used = [keep.read(arrays, name) for name in use]
    shapes = jax.eval_shape(function, *operands, *used)
    single = not isinstance(shapes, tuple)
    outs = (shapes,) if single else shapes
    outs = outs[: len(outs) - len(store)]
    count = len(operands)
    base = count + len(after)
    first_out = base + len(names)

    def body(*refs):
        kept = dict(zip(names, refs[base:first_out]))
        kept_out = dict(zip(names, refs[first_out + len(outs) :]))
        values = [ref[...] for ref in refs[:count]] + [keep.read(kept, name) for name in use]
        results = function(*values)
        results = (results,) if single else results
        for ref, result in zip(refs[first_out:], results[: len(outs)]):
            ref[...] = result
        for name, result in zip(store, results[len(outs) :]):
            bank, start, _ = keep.slots[name]
            kept_out[bank][pl.ds(start, result.shape[0]), :] = result

    held = [arrays[name] for name in names]
    aliases = {base + index: len(outs) + index for index in range(len(names))}
    results = call(
        body, (*operands, *after, *held), (*outs, *held), in_hbm=range(count, base), flops=flops,
        aliases=aliases,
    )
    arrays.update(zip(names, results[len(outs) :]))
    results = results[: len(outs)]
    return results[0] if single and results else tuple(results)


class Keep:
    def __init__(self):
        self.arrays, self.slots, self.rows = {}, {}, {}

    def plan(self, bank, sizes):
        self.rows[bank] = 0
        for name, size in sizes:
            self.slots[name] = (bank, self.rows[bank], size)
            self.rows[bank] += -(-size // 8) * 8

    def place(self, name):
        _, start, size = self.slots[name]
        return pl.ds(start, size)

    def read(self, arrays, name):
        name, wanted = name if isinstance(name, tuple) else (name, None)
        if name in self.slots:
            bank, start, size = self.slots[name]
            return arrays[bank][start : start + (wanted or size), :]
        return arrays[name][...]


def floats(*shape):
    return jax.ShapeDtypeStruct(shape, jnp.float32)


class Layout:
    def __init__(self, n):
        m = n - 1
        self.n, self.m = n, m
        self.block = n * m
        self.ring_rows = 4 * self.block
        flat = (n - 2) ** 2
        self.flat = -(-flat // 8) * 8
        self.rows = self.ring_rows + 2 * self.flat
        self.y_rows = self.block + -(-n // 8) * 8
        self.x_rows = 4 * m + self.flat
        at = lambda i, j, k: (i * n + j) * n + k
        inner = range(1, m)
        order = [at(i, j, k) for j in (0, m) for i in range(n) for k in range(m)]
        for j, k in ((0, 0), (m, m)):
            for i in range(n):
                order += [at(i, x, k) for x in inner] + [at(i, j, m)]
        for i in (0, m):
            order += [at(i, j, k) for j in inner for k in inner]
            order += [-1] * (self.flat - flat)
        self.order = np.array(order, np.int32)
        self.inner = np.array([at(i, j, k) for i in inner for j in inner for k in inner], np.int32)
        share = np.zeros((self.rows, 1), np.float32)
        for row, node in enumerate(order):
            if node >= 0:
                place = (node // (n * n), node // n % n, node % n)
                share[row] = 0.5 ** sum(x in (0, m) for x in place)
        self.share = share

    def blocks(self, ring):
        return [ring[s * self.block : (s + 1) * self.block] for s in range(4)]

    def row_in_tile(self, block):
        return lax.broadcasted_iota(jnp.int32, block.shape, 0) % self.m

    def fold_z(self, ring, below, above):
        first, last, low, high = self.blocks(ring)
        below, above = self.blocks(below), self.blocks(above)
        row = self.row_in_tile(first)
        start, end = row == 0, row == self.m - 1
        back = lambda x: roll_rows(x, x.shape[0] - (self.m - 1))
        ahead = lambda x: roll_rows(x, self.m - 1)
        zero = jnp.zeros_like(first)
        first = first + jnp.where(start, back(below[2]), zero)
        last = last + jnp.where(start, back(below[3]), zero)
        low = low + jnp.where(end, ahead(above[0]), below[3])
        high = high + jnp.where(end, ahead(above[1]), above[2])
        return jnp.concatenate([first, last, low, high], axis=0)

    def side(self, block, corners):
        lanes = block.shape[1]
        rows = corners.reshape(self.n, self.m, lanes)[:, self.m - 1, :]
        fill = jnp.zeros((self.y_rows - self.block - self.n, lanes), block.dtype)
        return jnp.concatenate([block, rows, fill], axis=0)

    def sides_y(self, ring):
        first, last, low, high = self.blocks(ring)
        return self.side(first, low), self.side(last, high)

    def fold_y(self, ring, below, above):
        first, last, low, high = self.blocks(ring)
        lanes = ring.shape[1]
        end = self.row_in_tile(first) == self.m - 1

        def ends(message):
            rows = message[self.block : self.block + self.n].reshape(self.n, 1, lanes)
            wide = jnp.broadcast_to(rows, (self.n, self.m, lanes)).reshape(self.block, lanes)
            return jnp.where(end, wide, jnp.zeros_like(wide))

        first = first + below[: self.block]
        low = low + ends(below)
        last = last + above[: self.block]
        high = high + ends(above)
        return jnp.concatenate([first, last, low, high], axis=0)

    def sides_x(self, ring, flat):
        m, block = self.m, self.block
        low = [ring[s * block : s * block + m] for s in range(4)] + [flat[: self.flat]]
        high = [ring[(s + 1) * block - m : (s + 1) * block] for s in range(4)] + [flat[self.flat :]]
        return jnp.concatenate(low, axis=0), jnp.concatenate(high, axis=0)

    def fold_x(self, ring, flat, below, above):
        m, block = self.m, self.block
        parts = []
        for s in range(4):
            parts += [
                ring[s * block : s * block + m] + below[s * m : (s + 1) * m],
                ring[s * block + m : (s + 1) * block - m],
                ring[(s + 1) * block - m : (s + 1) * block] + above[s * m : (s + 1) * m],
            ]
        parts += [flat[: self.flat] + below[4 * m :], flat[self.flat :] + above[4 * m :]]
        return jnp.concatenate(parts, axis=0)


def roll_rows(value, shift):
    if PALLAS:
        return pltpu.roll(value, shift, 0)
    return jnp.roll(value, shift, axis=0)


def shifted(value, axis, step):
    size = lax.axis_size(axis)
    return lax.ppermute(value, axis, [(i, (i + step) % size) for i in range(size)])


def both_ways(low, high, axis):
    return shifted(high, axis, 1), shifted(low, axis, -1)


def cat(parts):
    return parts[0] if len(parts) == 1 else jnp.concatenate(parts, axis=0)


def packed(layout, *fields):
    rings, rows = layout.ring_rows, layout.rows
    return cat([f[:rings] for f in fields]), cat([f[rings:rows] for f in fields])


def steps_of(axis):
    size = lax.axis_size(axis)
    return [1] if size == 2 else [1, size - 1, *range(2, size - 1)]


def assemble(
    layout, count, shares, rings, flats, function, keep, use=(), store=(), beside_y=None, beside_x=None
):
    ring_rows, flat_rows = layout.ring_rows, layout.rows - layout.ring_rows
    split = lambda value, size: [value[i * size : (i + 1) * size] for i in range(count)]
    column, slab = shares

    steps = steps_of("gz")
    sums = rings[count * ring_rows :] if len(steps) > 2 else None
    others = [shifted(rings, "gz", step) for step in steps[:2]]
    others += [shifted(sums, "gz", step) for step in steps[2:]]
    near = min(2, len(steps))

    def after_z(rings, flats, *others):
        done, low, high = [], [], []
        parts = [split(value, ring_rows) for value in (rings, others[0], others[near - 1])]
        for ring, below, above in zip(*parts):
            if near == 1:
                above = below
            ring = layout.fold_z(ring, below, above)
            sides = layout.sides_y(ring)
            done.append(ring)
            low.append(sides[0])
            high.append(sides[1])
        own = rings[count * ring_rows :]
        for index, other in enumerate(others):
            own = own + (other[count * ring_rows :] if index < near else other)
        return cat([*low, own]), cat([*high, own]), own, cat([*done, flats])

    work = ("work", count * layout.rows)
    low, high, own = run(after_z, rings, flats, *others, keep=keep, store=("work",))
    below, above = both_ways(low, high, "gy")
    steps = steps_of("gy")
    far = [shifted(own, "gy", step) for step in steps[2:]]
    ties = beside_y() if beside_y else ()

    def all_parts(own, below, above, far, edge, steps):
        parts = [own, below[edge:]]
        return parts + ([above[edge:]] if len(steps) > 1 else []) + list(far)

    def merged(chosen, parts, size):
        plain = sum(part[size:] for part in parts)
        wide = cat([part[:size] for part in parts])
        return pick(chosen[:, : wide.shape[0]].astype(jnp.bfloat16), wide), plain

    def after_y(below, above, own, *rest):
        far, (both, chosen) = rest[:-2], rest[-2:]
        done, low, high = [], [], []
        rings, flats = both[: count * ring_rows], both[count * ring_rows :]
        edge = count * layout.y_rows
        parts = (
            split(rings, ring_rows), split(flats, flat_rows), split(below[:edge], layout.y_rows),
            split(above[:edge], layout.y_rows),
        )
        for ring, flat, first, last in zip(*parts):
            ring = layout.fold_y(ring, first, last)
            sides = layout.sides_x(ring, flat)
            done.append(ring)
            low.append(sides[0])
            high.append(sides[1])
        own = cat(merged(chosen, all_parts(own, below, above, far, edge, steps), column))
        return cat([*low, own]), cat([*high, own]), own, cat([*done, flats])

    low, high, own = run(
        after_y, below, above, own, *far, after=ties, keep=keep, use=(work, "to_slab"), store=("work",)
    )
    below, above = both_ways(low, high, "gx")
    steps = steps_of("gx")
    far = [shifted(own, "gx", step) for step in steps[2:]]
    ties = beside_x() if beside_x else ()

    def after_x(below, above, own, *rest):
        far, (both, chosen), rest = rest[: len(steps) - 2], rest[len(steps) - 2 : len(steps)], rest[len(steps) :]
        rings, flats = both[: count * ring_rows], both[count * ring_rows :]
        edge = count * layout.x_rows
        parts = (
            split(rings, ring_rows), split(flats, flat_rows), split(below[:edge], layout.x_rows),
            split(above[:edge], layout.x_rows),
        )
        sums = merged(chosen, all_parts(own, below, above, far, edge, steps), slab)
        return function(*[layout.fold_x(*values) for values in zip(*parts)], *sums, *rest)

    return run(
        after_x, below, above, own, *far, after=ties, keep=keep, use=(work, "to_all", *use), store=store
    )


def parts_of(value):
    high = value.astype(jnp.bfloat16)
    rest = value - high.astype(jnp.float32)
    middle = rest.astype(jnp.bfloat16)
    low = (rest - middle.astype(jnp.float32)).astype(jnp.bfloat16)
    return high, middle, low


def pick(left, right, contract=(1, 0)):
    dims = (((contract[0],), (contract[1],)), ((), ()))
    if left.dtype == jnp.bfloat16:
        pairs = [(left, part) for part in parts_of(right)]
    else:
        pairs = [(part, right) for part in parts_of(left)]
    terms = [lax.dot_general(a, b, dims, preferred_element_type=jnp.float32) for a, b in pairs]
    return terms[0] + terms[1] + terms[2]


def one_hot_rows(column, count):
    lanes = lax.broadcasted_iota(jnp.int32, (column.shape[0], count), 1).astype(jnp.float32)
    return jnp.where(lanes == column, 1.0, 0.0).astype(jnp.bfloat16)


def one_hot_columns(row, count):
    places = lax.broadcasted_iota(jnp.int32, (count, row.shape[1]), 0).astype(jnp.float32)
    return jnp.where(places == row, 1.0, 0.0).astype(jnp.bfloat16)


def as_column(row):
    return jnp.broadcast_to(row, (8, row.shape[1])).T[:, :1]


def up(value, step):
    return -(-value // step) * step


def coarse_tables(counts, constraints):
    x, y, z = counts
    total = x * y * z

    def number(kind, i, j, k):
        return kind * total + (i % x * y + j % y) * z + k % z

    def own(a, b, c):
        two = (0, 1)
        listed = [number(0, a + i, b + j, c + k) for i in two for j in two for k in two]
        listed += [number(1, a, b + j, c + k) for j in two for k in two]
        listed += [number(2, a + i, b, c + k) for i in two for k in two]
        return listed + [number(3, a + i, b + j, c) for i in two for j in two]

    def unique(lists, pad):
        listed = sorted(set(sum(lists, [])))
        return listed + [pad] * (up(len(listed), 8) - len(listed))

    column = lambda a, b, pad: unique([own(a, b, c) for c in range(z)], pad)
    slab = lambda a, pad: unique([own(a, b, c) for b in range(y) for c in range(z)], pad)
    back_y = [0] + steps_of("gy")
    back_x = [0] + steps_of("gx")
    rows = []
    for a in range(x):
        for b in range(y):
            for c in range(z):
                first = own(a, b, c)
                rows.append([
                    first + [-1] * (constraints - len(first)), column(a, b, -2),
                    sum([column(a, (b - s) % y, -3) for s in back_y], []), slab(a, -4),
                    sum([slab((a - s) % x, -5) for s in back_x], []),
                ])
    starts, width = [], 0
    for listed in rows[0]:
        starts.append(width)
        width += up(len(listed), 128)
    table = np.full((total, width), -9, np.float32)
    for row, lists in zip(table, rows):
        for start, listed in zip(starts, lists):
            row[start : start + len(listed)] = listed
    sizes = [len(listed) for listed in rows[0]]
    return table, starts, sizes


def eliminate(matrix, pivots):
    count = matrix.shape[0]
    rows = lax.broadcasted_iota(jnp.int32, (8, count), 0)
    lanes = lax.broadcasted_iota(jnp.int32, (1, count), 1)
    for k in pivots:
        tile = k // 8 * 8
        column = jnp.take_along_axis(matrix, jnp.full(matrix.shape, k, jnp.int32), axis=1)
        row = jnp.where(lanes == k, 1.0, matrix[k : k + 1, :]) / column[k : k + 1, :]
        matrix = jnp.where(lanes == k, 0.0, matrix) - column * row
        own = jnp.where(rows == k - tile, row, matrix[tile : tile + 8])
        parts = [matrix[:tile], own, matrix[tile + 8 :]]
        matrix = jnp.concatenate([part for part in parts if part.shape[0]], axis=0)
    return matrix


def local(element_load, local_matrix, dirichlet_inverse, neumann_inverse, coarse_basis):
    n = element_load.shape[0]
    lanes = element_load.shape[3]
    nodes = n**3
    layout = Layout(n)
    inside = (n - 2) ** 3
    primal = coarse_basis.shape[3]
    counts = [lax.axis_size(axis) for axis in AXES]
    devices = counts[0] * counts[1] * counts[2]
    coarse = 4 * devices
    chunk = -(-primal // 8) * 8
    rows = layout.rows
    table, starts, sizes = coarse_tables(counts, chunk)
    shares = column, slab = sizes[1], sizes[3]
    rides = coarse == lanes
    own_table = jnp.asarray(table)
    places = np.stack([layout.order.astype(np.float32), layout.share[:, 0]])
    places = jnp.asarray(np.pad(places, ((0, 6), (0, 0))))
    pairs = [(i, j) for i in range(n) for j in range(n)]
    inner_pairs = [(i, j) for i in range(1, n - 1) for j in range(1, n - 1)]
    deep = n - 2

    def part(loads, chosen, *extra):
        mapped = pick(chosen[:, :chunk].astype(jnp.bfloat16), loads)
        fill = jnp.zeros((PLAIN - sum(rows.shape[0] for rows in extra), lanes), jnp.float32)
        return cat([mapped, *extra, fill])

    count = 1 + -(-coarse // lanes)
    ring_rows = layout.ring_rows
    names = ("condensed", "load", "residual", "field0", "image0", "image0_sum", "load_sum", "field1")
    keep = Keep()
    keep.plan(
        "bank",
        [("tau", 8), ("totals", 8), ("work", max(count, 2) * rows)] + [(name, rows) for name in names],
    )
    keep.plan("picks", [("to_column", column), ("to_slab", slab), ("to_all", coarse)])
    pick_lanes = up(max(sizes), 128)
    keep.plan(
        "matrices", [("schur", rows), ("scaled", rows), ("coupling", inside), ("weighted", chunk)]
    )

    def start(
        load, matrix, inverse, basis_in, places, own_table,
        bank, rings, flats, weighted, coarse_rows, picks,
        natural, load_inside, begun, begun_natural,
    ):
        order = places[0:1, :]
        surface = one_hot_rows(as_column(order), nodes)
        across = one_hot_columns(order, nodes)
        for i, j in pairs:
            natural[pl.ds((i * n + j) * n, n), :] = load[i, j]
        for index, (i, j) in enumerate(inner_pairs):
            load_inside[pl.ds(index * deep, deep), :] = load[i, j, pl.ds(1, deep), :]
        begun[...] = dot(inverse[0, 0, 0], load_inside[...])
        tau = jnp.sum(load_inside[...] * begun[...], axis=0, keepdims=True)
        begun_natural[...] = jnp.zeros_like(begun_natural)
        for index, (i, j) in enumerate(inner_pairs):
            begun_natural[pl.ds((i * n + j) * n + 1, deep), :] = begun[pl.ds(index * deep, deep), :]
        basis = jnp.concatenate(
            [basis_in[0, 0, 0], jnp.zeros((chunk - primal, nodes), jnp.float32)], axis=0
        )
        weighted[...] = pick(basis, across) * places[1:2, :]
        me = own_table[pl.ds(lax.axis_index(AXES), 1), :]
        lists = [me[:, s : s + up(size, 128)] for s, size in zip(starts, sizes)]
        own = one_hot_rows(as_column(lists[0])[:chunk], coarse)

        def match(name, targets, sources, size):
            found = jnp.where(targets == sources, 1.0, 0.0)
            lane = lax.broadcasted_iota(jnp.int32, found.shape, 1)
            found = jnp.where(lane < size, found, 0.0)
            picks[keep.place(name), pl.ds(0, found.shape[1])] = found
            return found

        to_column = match("to_column", as_column(lists[1])[:column], lists[0], chunk)
        match("to_slab", as_column(lists[3])[:slab], lists[2], sizes[2])
        every = lax.broadcasted_iota(jnp.int32, (coarse, 1), 0).astype(jnp.float32)
        match("to_all", every, lists[4], sizes[4])
        spread = pick(weighted[...], own, (0, 0))
        wide = jnp.concatenate([basis, jnp.zeros((128 - chunk, nodes), jnp.float32)], axis=0).T
        images = dot(matrix[0, 0, 0], jnp.concatenate([begun_natural[...], wide], axis=1))
        both = jnp.concatenate([natural[...], natural[...] - images[:, :lanes]], axis=1)
        both = pick(surface, both)
        condensed = both[:, lanes:]
        for name, value in (
            ("load", both[:, :lanes]), ("condensed", condensed),
            ("tau", jnp.broadcast_to(tau, (8, lanes))),
        ):
            bank[keep.place(name), :] = value
        fields = [condensed] + [spread[:, s : s + lanes] for s in range(0, coarse, lanes)]
        ringed, flats[...] = packed(layout, *fields)
        coarse_local = dot(basis, images[:, lanes:])
        spread_rows = pick(coarse_local[:, :chunk], own)
        coarse_rows[...] = spread_rows
        if rides:
            ridden = part(spread_rows, to_column)
        else:
            ridden = jnp.zeros((column + PLAIN, lanes), jnp.float32)
        rings[...] = cat([ringed, ridden])

    bank, rings, flats, weighted, coarse_rows, picks = call(
        start,
        (element_load, local_matrix, dirichlet_inverse, coarse_basis, places, own_table),
        (
            floats(keep.rows["bank"], lanes), floats(count * ring_rows + column + PLAIN, lanes),
            floats(count * (rows - ring_rows), lanes), floats(chunk, rows),
            floats(chunk, coarse), floats(keep.rows["picks"], pick_lanes),
        ),
        scratch=[
            VMEM((nodes, lanes), jnp.float32), VMEM((inside, lanes), jnp.float32),
            VMEM((inside, lanes), jnp.float32), VMEM((nodes, lanes), jnp.float32),
        ],
    )
    element_load, local_matrix, dirichlet_inverse = lax.optimization_barrier(
        (element_load, local_matrix, dirichlet_inverse)
    )

    keep.arrays.update(bank=bank, picks=picks)

    def reorder(neumann, places):
        order, share = places[0:1, :], places[1:2, :]
        across = one_hot_columns(order, nodes)
        surface = one_hot_rows(as_column(order), nodes)
        return pick(surface, pick(neumann[0, 0, 0], across)) * as_column(share) * share

    def condense(matrix, inverse, places, weighted, out):
        places = places[...]
        order = places[0:1, :]
        picked = pick(matrix[0, 0, 0], one_hot_columns(order, nodes))
        surface = one_hot_rows(as_column(order), nodes)
        within = pick(surface, picked)
        coupling = jnp.concatenate(
            [picked[(i * n + j) * n + 1 : (i * n + j) * n + 1 + deep] for i, j in inner_pairs], axis=0
        )
        out[keep.place("coupling"), :] = coupling
        out[keep.place("weighted"), :] = weighted[...]
        out[keep.place("schur"), :] = within - dot(coupling, dot(inverse[0, 0, 0], coupling), (0, 0))

    def make_schur():
        (keep.arrays["matrices"],) = call(
            condense, (local_matrix, dirichlet_inverse, places, weighted),
            (floats(keep.rows["matrices"], rows),), flops=FILL,
        )
        return ()

    def make_scaled():
        run(reorder, neumann_inverse, places, flops=FILL, keep=keep, store=("scaled",))
        return ()

    step = coarse // PIECES

    def invert(first, last):
        for piece in range(first, last):

            def eliminated(matrix, piece=piece):
                return eliminate(matrix, range(piece * step, (piece + 1) * step))

            keep.arrays["coarse"] = run(eliminated, keep.arrays["coarse"], flops=FILL)

    def invert_early():
        if rides:
            invert(0, PIECES - 1)
        return ()

    def finish_inverse():
        if rides:
            invert(PIECES - 1, PIECES)
        keep.arrays["lift"] = run(dot, keep.arrays.pop("spread"), keep.arrays.pop("coarse"))
        return ()

    def other_inverse():
        spread_rows = jnp.broadcast_to(coarse_rows[None], (devices, *coarse_rows.shape))
        gathered = lax.all_to_all(spread_rows, AXES, 0, 0, tiled=True).reshape(-1, coarse)
        ids = jnp.asarray(table[:, :chunk].reshape(1, -1))
        summed = run(lambda ids, rows: pick(one_hot_columns(ids, coarse), rows), ids, gathered)
        factor = jnp.linalg.cholesky(summed)
        eye = jnp.eye(coarse, dtype=jnp.float32)
        return jax.scipy.linalg.cho_solve((factor, True), eye)

    def neumann_step(field, scaled, weighted):
        return dot(scaled, field), dot(weighted, field)

    def sent(field, loads, chosen, *extra):
        ringed, flats = packed(layout, field)
        return cat([ringed, part(loads, chosen, *extra)]), flats

    def first(field, *rest):
        pieces, (summed, _, weighted, scaled, chosen) = rest[:-5], rest[-5:]
        mapped, loads = neumann_step(field, scaled, weighted)
        spread = jnp.concatenate(pieces, axis=1) if len(pieces) > 1 else pieces[0]
        return (spread, summed, *sent(mapped, loads, chosen), field)

    keep.arrays["spread"], keep.arrays["coarse"], rings, flats = assemble(
        layout, count, shares, rings, flats, first, keep, ("weighted", "scaled", "to_column"),
        ("residual",), make_schur, make_scaled,
    )
    if not rides:
        keep.arrays["coarse"] = other_inverse()

    def apply_first(mapped, summed, _, condensed, tau, load, schur, lift):
        field = mapped + dot(lift, summed)
        image = dot(schur, field)
        energy = tau[:1] + jnp.sum(condensed * field, axis=0, keepdims=True)
        curvature = tau[:1] + jnp.sum(field * image, axis=0, keepdims=True)
        fill = jnp.zeros((6, lanes), jnp.float32)
        ringed, flats = packed(layout, image, load)
        ridden = jnp.zeros((column + PLAIN, lanes), jnp.float32)
        sums = jnp.concatenate([energy, curvature, fill], axis=0)
        return cat([ringed, ridden]), flats, field, image, sums

    rings, flats = assemble(
        layout, 1, shares, rings, flats, apply_first, keep,
        ("condensed", "tau", "load", "schur", "lift"), ("field0", "image0", "totals"), invert_early,
        finish_inverse,
    )

    def second(image, load, summed, _, sums, scaled, weighted, chosen):
        mapped, loads = neumann_step(image, scaled, weighted)
        return (*sent(mapped, loads, chosen, sums[:2]), image, load)

    rings, flats = assemble(
        layout, 2, shares, rings, flats, second, keep,
        ("totals", "scaled", "weighted", "to_column"), ("image0_sum", "load_sum"),
    )

    def apply_second(mapped, summed, totals, schur, condensed, tau, field0, image0, lift):
        field = mapped + dot(lift, summed)
        image = dot(schur, field)
        step = totals[:1] / totals[1:2]
        rest = 1.0 - step
        direction = field0 - step * field
        direction_image = image0 - step * image
        energy = rest * rest * tau[:1] + jnp.sum(
            (condensed - step * image0) * direction, axis=0, keepdims=True
        )
        curvature = rest * rest * tau[:1] + jnp.sum(
            direction * direction_image, axis=0, keepdims=True
        )
        cross = rest * tau[:1] + jnp.sum(direction * image0, axis=0, keepdims=True)
        ringed, flats = packed(layout, image)
        ridden = jnp.zeros((column, lanes), jnp.float32)
        fill = jnp.zeros((PLAIN - 3, lanes), jnp.float32)
        return cat([ringed, ridden, energy, curvature, cross, fill]), flats, field, totals

    rings, flats = assemble(
        layout, 1, shares, rings, flats, apply_second, keep,
        ("schur", "condensed", "tau", "field0", "image0", "lift"), ("field1", "totals"),
    )

    def put(out, surface, deep_rows, load, factor):
        m, block = n - 1, layout.block
        for i in range(n):
            for s, j in ((0, 0), (1, m)):
                out[i, j, pl.ds(0, m), :] = surface[pl.ds(s * block + i * m, m), :]
                out[i, j, pl.ds(m, 1), :] = surface[pl.ds((s + 2) * block + i * m + m - 1, 1), :]
            for j in range(1, m):
                for s, k in ((2, 0), (3, m)):
                    out[i, j, pl.ds(k, 1), :] = surface[pl.ds(s * block + i * m + j - 1, 1), :]
                if i in (0, m):
                    at = layout.ring_rows + (layout.flat if i else 0) + (j - 1) * deep
                    out[i, j, pl.ds(1, deep), :] = surface[pl.ds(at, deep), :]
                elif deep_rows is None:
                    out[i, j, pl.ds(1, deep), :] = factor * load[i, j, pl.ds(1, deep), :]
                else:
                    at = ((i - 1) * deep + j - 1) * deep
                    out[i, j, pl.ds(1, deep), :] = deep_rows[pl.ds(at, deep), :]

    def solve_inside(bank, matrices, inverse, load, out, inner_load):
        for index, (i, j) in enumerate(inner_pairs):
            inner_load[pl.ds(index * deep, deep), :] = load[i, j, pl.ds(1, deep), :]
        fields = jnp.concatenate([bank[keep.place("field0"), :], bank[keep.place("field1"), :]], axis=1)
        loads = jnp.concatenate([inner_load[...], inner_load[...]], axis=1)
        right = loads - dot(matrices[keep.place("coupling"), :], fields)
        out[...] = dot(inverse[0, 0, 0], right)

    def finish_inside():
        (keep.arrays["deep"],) = call(
            solve_inside, (keep.arrays["bank"], keep.arrays["matrices"], dirichlet_inverse, element_load),
            (floats(inside, 2 * lanes),), scratch=[VMEM((inside, lanes), jnp.float32)], flops=FILL,
        )
        return ()

    def leftover(image1, _, sums, totals, field0, field1, image0, residual, load_sum):
        energy, curvature = totals[:1], totals[1:2]
        step = energy / curvature
        energy_next, curvature_next, cross = sums[:1], sums[1:2], sums[2:3]
        ratio = energy_next / energy
        curvature_next = curvature_next + 2.0 * ratio * cross + ratio * ratio * curvature
        step_next = energy_next / curvature_next
        first = step + step_next * (1.0 + ratio)
        second = -step_next * step
        spill = load_sum - residual
        residual_surface = load_sum - first * (image0 + spill) - second * (image1 + spill)
        fill = jnp.zeros((6, lanes), jnp.float32)
        weights = jnp.concatenate([first, second, fill], axis=0)
        return first * field0 + second * field1, residual_surface, weights

    solution_surface, residual_surface, weights = assemble(
        layout, 1, shares, rings, flats, leftover, keep,
        ("totals", "field0", "field1", "image0_sum", "residual", "load_sum"), (), finish_inside,
    )

    def place(solution_surface, residual_surface, weights, both, load, one, two, deep_rows):
        first, second = weights[0:1, :], weights[1:2, :]
        deep_rows[...] = first * both[:, :lanes] + second * both[:, lanes:]
        put(one, solution_surface, deep_rows, None, None)
        put(two, residual_surface, None, load, 1.0 - first - second)

    shape = floats(*element_load.shape)
    solution_out, residual_out = call(
        place, (solution_surface, residual_surface, weights, keep.arrays["deep"], element_load),
        (shape, shape), scratch=[VMEM((inside, lanes), jnp.float32)],
    )
    return solution_out, residual_out


def solution(mesh):
    in_specs = (
        P("gx", "gy", "gz", None),
        P("gx", "gy", "gz", None, None),
        P("gx", "gy", "gz", None, None),
        P("gx", "gy", "gz", None, None),
        P("gx", "gy", "gz", None, None),
    )
    out_specs = (P("gx", "gy", "gz", None), P("gx", "gy", "gz", None))
    return jax.shard_map(local, mesh=mesh, in_specs=in_specs, out_specs=out_specs, check_vma=False)
```

```python
import jax
import jax.numpy as jnp
import numpy as np
from jax import lax
from jax.experimental import pallas as pl
from jax.experimental.pallas import tpu as pltpu
from jax.sharding import PartitionSpec as P

AXES = ("gx", "gy", "gz")
HIGHEST = lax.Precision.HIGHEST
PALLAS = True
LIMIT = 24 * 2**20
VMEM = pltpu.VMEM
PIECES = 4
PLAIN = 8
FILL = 10**8


def dot(left, right, contract=(1, 0)):
    dims = (((contract[0],), (contract[1],)), ((), ()))
    return lax.dot_general(
        left, right, dims, precision=HIGHEST, preferred_element_type=jnp.float32
    )


def whole(count):
    return [pl.BlockSpec(memory_space=VMEM)] * count


def call(body, operands, outs, scratch=(), in_hbm=(), flops=10**6, aliases=None):
    places = whole(len(operands))
    for index in in_hbm:
        places[index] = pl.BlockSpec(memory_space=pl.ANY)
    size = sum(4 * np.prod(x.shape) for x in (*operands, *outs))
    return pl.pallas_call(
        body,
        out_shape=[jax.ShapeDtypeStruct(x.shape, x.dtype) for x in outs],
        in_specs=places,
        out_specs=whole(len(outs)),
        scratch_shapes=scratch,
        input_output_aliases=aliases or {},
        compiler_params=pltpu.CompilerParams(vmem_limit_bytes=LIMIT),
        cost_estimate=pl.CostEstimate(flops=flops, bytes_accessed=int(size), transcendentals=0),
    )(*operands)


def run(function, *operands, flops=10**6, after=(), keep=None, use=(), store=()):
    arrays = {} if keep is None else keep.arrays
    names = list(arrays)
    used = [keep.read(arrays, name) for name in use]
    shapes = jax.eval_shape(function, *operands, *used)
    single = not isinstance(shapes, tuple)
    outs = (shapes,) if single else shapes
    outs = outs[: len(outs) - len(store)]
    count = len(operands)
    base = count + len(after)
    first_out = base + len(names)

    def body(*refs):
        kept = dict(zip(names, refs[base:first_out]))
        kept_out = dict(zip(names, refs[first_out + len(outs) :]))
        values = [ref[...] for ref in refs[:count]] + [keep.read(kept, name) for name in use]
        results = function(*values)
        results = (results,) if single else results
        for ref, result in zip(refs[first_out:], results[: len(outs)]):
            ref[...] = result
        for name, result in zip(store, results[len(outs) :]):
            bank, start, _ = keep.slots[name]
            kept_out[bank][pl.ds(start, result.shape[0]), :] = result

    held = [arrays[name] for name in names]
    aliases = {base + index: len(outs) + index for index in range(len(names))}
    results = call(
        body, (*operands, *after, *held), (*outs, *held), in_hbm=range(count, base), flops=flops,
        aliases=aliases,
    )
    arrays.update(zip(names, results[len(outs) :]))
    results = results[: len(outs)]
    return results[0] if single and results else tuple(results)


class Keep:
    def __init__(self):
        self.arrays, self.slots, self.rows = {}, {}, {}

    def plan(self, bank, sizes):
        self.rows[bank] = 0
        for name, size in sizes:
            self.slots[name] = (bank, self.rows[bank], size)
            self.rows[bank] += -(-size // 8) * 8

    def place(self, name):
        _, start, size = self.slots[name]
        return pl.ds(start, size)

    def read(self, arrays, name):
        name, wanted = name if isinstance(name, tuple) else (name, None)
        if name in self.slots:
            bank, start, size = self.slots[name]
            return arrays[bank][start : start + (wanted or size), :]
        return arrays[name][...]


def floats(*shape):
    return jax.ShapeDtypeStruct(shape, jnp.float32)


class Layout:
    def __init__(self, n):
        m = n - 1
        self.n, self.m = n, m
        self.block = n * m
        self.ring_rows = 4 * self.block
        flat = (n - 2) ** 2
        self.flat = -(-flat // 8) * 8
        self.rows = self.ring_rows + 2 * self.flat
        self.y_rows = self.block + -(-n // 8) * 8
        self.x_rows = 4 * m + self.flat
        at = lambda i, j, k: (i * n + j) * n + k
        inner = range(1, m)
        order = [at(i, j, k) for j in (0, m) for i in range(n) for k in range(m)]
        for j, k in ((0, 0), (m, m)):
            for i in range(n):
                order += [at(i, x, k) for x in inner] + [at(i, j, m)]
        for i in (0, m):
            order += [at(i, j, k) for j in inner for k in inner]
            order += [-1] * (self.flat - flat)
        self.order = np.array(order, np.int32)
        self.inner = np.array([at(i, j, k) for i in inner for j in inner for k in inner], np.int32)
        share = np.zeros((self.rows, 1), np.float32)
        for row, node in enumerate(order):
            if node >= 0:
                place = (node // (n * n), node // n % n, node % n)
                share[row] = 0.5 ** sum(x in (0, m) for x in place)
        self.share = share

    def blocks(self, ring):
        return [ring[s * self.block : (s + 1) * self.block] for s in range(4)]

    def row_in_tile(self, block):
        return lax.broadcasted_iota(jnp.int32, block.shape, 0) % self.m

    def fold_z(self, ring, below, above):
        first, last, low, high = self.blocks(ring)
        below, above = self.blocks(below), self.blocks(above)
        row = self.row_in_tile(first)
        start, end = row == 0, row == self.m - 1
        back = lambda x: roll_rows(x, x.shape[0] - (self.m - 1))
        ahead = lambda x: roll_rows(x, self.m - 1)
        zero = jnp.zeros_like(first)
        first = first + jnp.where(start, back(below[2]), zero)
        last = last + jnp.where(start, back(below[3]), zero)
        low = low + jnp.where(end, ahead(above[0]), below[3])
        high = high + jnp.where(end, ahead(above[1]), above[2])
        return jnp.concatenate([first, last, low, high], axis=0)

    def side(self, block, corners):
        lanes = block.shape[1]
        rows = corners.reshape(self.n, self.m, lanes)[:, self.m - 1, :]
        fill = jnp.zeros((self.y_rows - self.block - self.n, lanes), block.dtype)
        return jnp.concatenate([block, rows, fill], axis=0)

    def sides_y(self, ring):
        first, last, low, high = self.blocks(ring)
        return self.side(first, low), self.side(last, high)

    def fold_y(self, ring, below, above):
        first, last, low, high = self.blocks(ring)
        lanes = ring.shape[1]
        end = self.row_in_tile(first) == self.m - 1

        def ends(message):
            rows = message[self.block : self.block + self.n].reshape(self.n, 1, lanes)
            wide = jnp.broadcast_to(rows, (self.n, self.m, lanes)).reshape(self.block, lanes)
            return jnp.where(end, wide, jnp.zeros_like(wide))

        first = first + below[: self.block]
        low = low + ends(below)
        last = last + above[: self.block]
        high = high + ends(above)
        return jnp.concatenate([first, last, low, high], axis=0)

    def sides_x(self, ring, flat):
        m, block = self.m, self.block
        low = [ring[s * block : s * block + m] for s in range(4)] + [flat[: self.flat]]
        high = [ring[(s + 1) * block - m : (s + 1) * block] for s in range(4)] + [flat[self.flat :]]
        return jnp.concatenate(low, axis=0), jnp.concatenate(high, axis=0)

    def fold_x(self, ring, flat, below, above):
        m, block = self.m, self.block
        parts = []
        for s in range(4):
            parts += [
                ring[s * block : s * block + m] + below[s * m : (s + 1) * m],
                ring[s * block + m : (s + 1) * block - m],
                ring[(s + 1) * block - m : (s + 1) * block] + above[s * m : (s + 1) * m],
            ]
        parts += [flat[: self.flat] + below[4 * m :], flat[self.flat :] + above[4 * m :]]
        return jnp.concatenate(parts, axis=0)


def roll_rows(value, shift):
    if PALLAS:
        return pltpu.roll(value, shift, 0)
    return jnp.roll(value, shift, axis=0)


def shifted(value, axis, step):
    size = lax.axis_size(axis)
    return lax.ppermute(value, axis, [(i, (i + step) % size) for i in range(size)])


def both_ways(low, high, axis):
    return shifted(high, axis, 1), shifted(low, axis, -1)


def cat(parts):
    return parts[0] if len(parts) == 1 else jnp.concatenate(parts, axis=0)


def packed(layout, *fields):
    rings, rows = layout.ring_rows, layout.rows
    return cat([f[:rings] for f in fields]), cat([f[rings:rows] for f in fields])


def steps_of(axis):
    size = lax.axis_size(axis)
    return [1] if size == 2 else [1, size - 1, *range(2, size - 1)]


def assemble(
    layout, count, shares, rings, flats, function, keep, use=(), store=(), beside_z=None, beside_y=None,
    beside_x=None,
):
    ring_rows, flat_rows = layout.ring_rows, layout.rows - layout.ring_rows
    split = lambda value, size: [value[i * size : (i + 1) * size] for i in range(count)]
    column, slab = shares or (0, 0)
    far_steps = lambda axis: steps_of(axis)[2:] if shares else []
    picked = lambda name: (name,) if column else ()

    steps = [*steps_of("gz")[:2], *far_steps("gz")]
    sums = rings[count * ring_rows :] if len(steps) > 2 else None
    others = [shifted(rings, "gz", step) for step in steps[:2]]
    others += [shifted(sums, "gz", step) for step in steps[2:]]
    ties = beside_z() if beside_z else ()
    near = len(steps_of("gz")[:2])

    def after_z(rings, flats, *others):
        done, low, high = [], [], []
        parts = [split(value, ring_rows) for value in (rings, others[0], others[near - 1])]
        for ring, below, above in zip(*parts):
            if near == 1:
                above = below
            ring = layout.fold_z(ring, below, above)
            sides = layout.sides_y(ring)
            done.append(ring)
            low.append(sides[0])
            high.append(sides[1])
        if not shares:
            return cat(low), cat(high), cat([*done, flats])
        own = rings[count * ring_rows :]
        for index, other in enumerate(others):
            own = own + (other[count * ring_rows :] if index < near else other)
        return cat([*low, own]), cat([*high, own]), own, cat([*done, flats])

    work = ("work", count * layout.rows)
    low, high, *own = run(after_z, rings, flats, *others, after=ties, keep=keep, store=("work",))
    far = [shifted(own[0], "gy", step) for step in far_steps("gy")]
    below, above = both_ways(low, high, "gy")
    ties = beside_y() if beside_y else ()

    def all_parts(own, below, above, far, edge, axis):
        parts = [own, below[edge:]]
        return parts + ([above[edge:]] if len(steps_of(axis)) > 1 else []) + list(far)

    def merged(chosen, parts, size):
        plain = sum(part[size:] for part in parts)
        if not size:
            return (plain,)
        wide = cat([part[:size] for part in parts])
        return pick(chosen[0][:, : wide.shape[0]].astype(jnp.bfloat16), wide), plain

    def after_y(below, above, *rest):
        own, rest = rest[: len(own_y)], rest[len(own_y) :]
        far, both, chosen = rest[: len(far_y)], rest[len(far_y)], rest[len(far_y) + 1 :]
        done, low, high = [], [], []
        rings, flats = both[: count * ring_rows], both[count * ring_rows :]
        edge = count * layout.y_rows
        parts = (
            split(rings, ring_rows), split(flats, flat_rows), split(below[:edge], layout.y_rows),
            split(above[:edge], layout.y_rows),
        )
        for ring, flat, first, last in zip(*parts):
            ring = layout.fold_y(ring, first, last)
            sides = layout.sides_x(ring, flat)
            done.append(ring)
            low.append(sides[0])
            high.append(sides[1])
        if not shares:
            return cat(low), cat(high), cat([*done, flats])
        own = cat(merged(chosen, all_parts(own[0], below, above, far, edge, "gy"), column))
        return cat([*low, own]), cat([*high, own]), own, cat([*done, flats])

    own_y, far_y = own, far
    low, high, *own = run(
        after_y, below, above, *own, *far, after=ties, keep=keep, use=(work, *picked("to_slab")),
        store=("work",),
    )
    far = [shifted(own[0], "gx", step) for step in far_steps("gx")]
    below, above = both_ways(low, high, "gx")
    ties = beside_x() if beside_x else ()

    def after_x(below, above, *rest):
        own_x, rest = rest[: len(own)], rest[len(own) :]
        far_x, both, rest = rest[: len(far)], rest[len(far)], rest[len(far) + 1 :]
        chosen, rest = (rest[:1], rest[1:]) if column else ((), rest)
        rings, flats = both[: count * ring_rows], both[count * ring_rows :]
        edge = count * layout.x_rows
        parts = (
            split(rings, ring_rows), split(flats, flat_rows), split(below[:edge], layout.x_rows),
            split(above[:edge], layout.x_rows),
        )
        sums = ()
        if shares:
            sums = merged(chosen, all_parts(own_x[0], below, above, far_x, edge, "gx"), slab)
        return function(*[layout.fold_x(*values) for values in zip(*parts)], *sums, *rest)

    return run(
        after_x, below, above, *own, *far, after=ties, keep=keep,
        use=(work, *picked("to_all"), *use), store=store,
    )


def parts_of(value):
    high = value.astype(jnp.bfloat16)
    rest = value - high.astype(jnp.float32)
    middle = rest.astype(jnp.bfloat16)
    low = (rest - middle.astype(jnp.float32)).astype(jnp.bfloat16)
    return high, middle, low


def pick(left, right, contract=(1, 0)):
    dims = (((contract[0],), (contract[1],)), ((), ()))
    if left.dtype == jnp.bfloat16:
        pairs = [(left, part) for part in parts_of(right)]
    else:
        pairs = [(part, right) for part in parts_of(left)]
    terms = [lax.dot_general(a, b, dims, preferred_element_type=jnp.float32) for a, b in pairs]
    return terms[0] + terms[1] + terms[2]


def stacked(value):
    return jnp.concatenate(parts_of(value), axis=0)


def product(stack, right):
    rows, lanes = stack.shape[0] // 3, right.shape[1]
    high, middle, low = parts_of(right)
    times = lambda a, b: jnp.dot(a, b, preferred_element_type=jnp.float32)
    wide = times(stack[: 2 * rows], jnp.concatenate([high, middle], axis=1))
    small = wide[rows:, lanes:] + times(stack[:rows], low) + times(stack[2 * rows :], high)
    return wide[:rows, :lanes] + (wide[:rows, lanes:] + wide[rows:, :lanes] + small)


def runs_of(places):
    found, at = [], 0
    while at < len(places):
        if places[at] < 0:
            at += 1
            continue
        size, stride = 1, 1
        if at + 1 < len(places) and places[at + 1] > places[at]:
            stride = int(places[at + 1] - places[at])
            while at + size < len(places) and places[at + size] - places[at + size - 1] == stride:
                size += 1
            if size == 2 and stride > 1:
                size = 1
        found.append((at, int(places[at]), size, stride if size > 1 else 1))
        at += size
    return found


def one_hot_rows(column, count):
    lanes = lax.broadcasted_iota(jnp.int32, (column.shape[0], count), 1).astype(jnp.float32)
    return jnp.where(lanes == column, 1.0, 0.0).astype(jnp.bfloat16)


def one_hot_columns(row, count):
    places = lax.broadcasted_iota(jnp.int32, (count, row.shape[1]), 0).astype(jnp.float32)
    return jnp.where(places == row, 1.0, 0.0).astype(jnp.bfloat16)


def as_column(row):
    return jnp.broadcast_to(row, (8, row.shape[1])).T[:, :1]


def up(value, step):
    return -(-value // step) * step


def coarse_tables(counts, constraints):
    x, y, z = counts
    total = x * y * z

    def number(kind, i, j, k):
        return kind * total + (i % x * y + j % y) * z + k % z

    def own(a, b, c):
        two = (0, 1)
        listed = [number(0, a + i, b + j, c + k) for i in two for j in two for k in two]
        listed += [number(1, a, b + j, c + k) for j in two for k in two]
        listed += [number(2, a + i, b, c + k) for i in two for k in two]
        return listed + [number(3, a + i, b + j, c) for i in two for j in two]

    def unique(lists, pad):
        listed = sorted(set(sum(lists, [])))
        return listed + [pad] * (up(len(listed), 8) - len(listed))

    column = lambda a, b, pad: unique([own(a, b, c) for c in range(z)], pad)
    slab = lambda a, pad: unique([own(a, b, c) for b in range(y) for c in range(z)], pad)
    back_y = [0] + steps_of("gy")
    back_x = [0] + steps_of("gx")
    rows = []
    for a in range(x):
        for b in range(y):
            for c in range(z):
                first = own(a, b, c)
                rows.append([
                    first + [-1] * (constraints - len(first)), column(a, b, -2),
                    sum([column(a, (b - s) % y, -3) for s in back_y], []), slab(a, -4),
                    sum([slab((a - s) % x, -5) for s in back_x], []),
                ])
    starts, width = [], 0
    for listed in rows[0]:
        starts.append(width)
        width += up(len(listed), 128)
    table = np.full((total, width), -9, np.float32)
    for row, lists in zip(table, rows):
        for start, listed in zip(starts, lists):
            row[start : start + len(listed)] = listed
    sizes = [len(listed) for listed in rows[0]]
    return table, starts, sizes


def eliminate(matrix, pivots):
    count = matrix.shape[0]
    rows = lax.broadcasted_iota(jnp.int32, (8, count), 0)
    lanes = lax.broadcasted_iota(jnp.int32, (1, count), 1)
    for k in pivots[::2]:
        m, tile = k + 1, k // 8 * 8
        spread = lambda lane: jnp.take_along_axis(
            matrix, jnp.full(matrix.shape, lane, jnp.int32), axis=1
        )
        column0, column1 = spread(k), spread(m)
        a, b, d = column0[k:m], column1[k:m], column1[m : m + 1]
        scale = 1.0 / (a * d - b * b)
        here = (lanes == k) | (lanes == m)
        row0 = jnp.where(here, jnp.where(lanes == k, 1.0, 0.0), matrix[k:m, :])
        row1 = jnp.where(here, jnp.where(lanes == m, 1.0, 0.0), matrix[m : m + 1, :])
        new0 = (d * row0 - b * row1) * scale
        new1 = (a * row1 - b * row0) * scale
        matrix = jnp.where(here, 0.0, matrix) - column0 * new0 - column1 * new1
        own = jnp.where(rows == k - tile, new0, matrix[tile : tile + 8])
        own = jnp.where(rows == m - tile, new1, own)
        parts = [matrix[:tile], own, matrix[tile + 8 :]]
        matrix = jnp.concatenate([part for part in parts if part.shape[0]], axis=0)
    return matrix


def local(element_load, local_matrix, dirichlet_inverse, neumann_inverse, coarse_basis):
    n = element_load.shape[0]
    lanes = element_load.shape[3]
    nodes = n**3
    layout = Layout(n)
    inside = (n - 2) ** 3
    primal = coarse_basis.shape[3]
    counts = [lax.axis_size(axis) for axis in AXES]
    devices = counts[0] * counts[1] * counts[2]
    coarse = 4 * devices
    chunk = -(-primal // 8) * 8
    rows = layout.rows
    table, starts, sizes = coarse_tables(counts, chunk)
    shares = column, slab = sizes[1], sizes[3]
    rides = coarse == lanes
    own_table = jnp.asarray(table)
    places = np.stack([layout.order.astype(np.float32), layout.share[:, 0]])
    places = jnp.asarray(np.pad(places, ((0, 6), (0, 0))))
    pairs = [(i, j) for i in range(n) for j in range(n)]
    inner_pairs = [(i, j) for i in range(1, n - 1) for j in range(1, n - 1)]
    deep = n - 2


    count = 1 + -(-coarse // lanes)
    ring_rows = layout.ring_rows
    names = ("condensed", "load", "residual", "field0", "image0", "image0_sum", "load_sum", "field1")
    keep = Keep()
    keep.plan(
        "bank",
        [("tau", 8), ("totals", 8), ("work", max(count, 2) * rows)] + [(name, rows) for name in names],
    )
    keep.plan("picks", [("to_column", column), ("to_slab", slab), ("to_all", coarse)])
    pick_lanes = up(max(sizes), 128)
    loads_rows = up(rows + chunk, 16)

    def prepare(
        load, inverse, basis_in, places, own_table,
        natural, right, tau, weighted, spread, own_hot, basis, picks, load_inside, begun,
    ):
        order = places[0:1, :]
        across = one_hot_columns(order, nodes)
        for i, j in pairs:
            natural[pl.ds((i * n + j) * n, n), :] = load[i, j]
        for index, (i, j) in enumerate(inner_pairs):
            load_inside[pl.ds(index * deep, deep), :] = load[i, j, pl.ds(1, deep), :]
        begun[...] = dot(inverse[0, 0, 0], load_inside[...])
        tau[...] = jnp.broadcast_to(
            jnp.sum(load_inside[...] * begun[...], axis=0, keepdims=True), (8, lanes)
        )
        right[:, pl.ds(0, lanes)] = jnp.zeros((nodes, lanes), jnp.float32)
        for index, (i, j) in enumerate(inner_pairs):
            right[pl.ds((i * n + j) * n + 1, deep), pl.ds(0, lanes)] = begun[
                pl.ds(index * deep, deep), :
            ]
        basis[...] = jnp.concatenate(
            [basis_in[0, 0, 0], jnp.zeros((chunk - primal, nodes), jnp.float32)], axis=0
        )
        right[:, pl.ds(lanes, 128)] = jnp.concatenate(
            [basis[...], jnp.zeros((128 - chunk, nodes), jnp.float32)], axis=0
        ).T
        weighted[...] = pick(basis[...], across) * places[1:2, :]
        me = own_table[pl.ds(lax.axis_index(AXES), 1), :]
        lists = [me[:, s : s + up(size, 128)] for s, size in zip(starts, sizes)]
        own = one_hot_rows(as_column(lists[0])[:chunk], coarse)
        own_hot[...] = own.astype(jnp.float32)
        spread[...] = pick(weighted[...], own, (0, 0))

        def match(name, targets, sources, size):
            found = jnp.where(targets == sources, 1.0, 0.0)
            lane = lax.broadcasted_iota(jnp.int32, found.shape, 1)
            picks[keep.place(name), pl.ds(0, found.shape[1])] = jnp.where(lane < size, found, 0.0)

        match("to_column", as_column(lists[1])[:column], lists[0], chunk)
        match("to_slab", as_column(lists[3])[:slab], lists[2], sizes[2])
        every = lax.broadcasted_iota(jnp.int32, (coarse, 1), 0).astype(jnp.float32)
        match("to_all", every, lists[4], sizes[4])

    def part(loads, chosen, *extra):
        mapped = pick(chosen[:, :chunk].astype(jnp.bfloat16), loads)
        fill = jnp.zeros((PLAIN - sum(rows.shape[0] for rows in extra), lanes), jnp.float32)
        return cat([mapped, *extra, fill])

    moves = runs_of(list(layout.order))
    empty = runs_of([row if node < 0 else -1 for row, node in enumerate(layout.order)])

    def start(
        matrix, right, natural, tau, spread, own_hot, basis, picks,
        bank, rings, flats, coarse_rows, rest,
    ):
        images = dot(matrix[0, 0, 0], right[...])
        coarse_local = dot(basis[...], images[:, lanes:])
        rest[...] = natural[...] - images[:, :lanes]
        bank[keep.place("tau"), :] = tau[...]
        for name, source in (("load", natural), ("condensed", rest)):
            first = keep.slots[name][1]
            for _, row, size, _ in empty:
                bank[pl.ds(first + row, size), :] = jnp.zeros((size, lanes), jnp.float32)
            for at, row, size, stride in moves:
                bank[pl.ds(first + at, size), :] = source[pl.ds(row, size, stride), :]
        fields = [bank[keep.place("condensed"), :]]
        fields += [spread[:, s : s + lanes] for s in range(0, coarse, lanes)]
        ringed, flats[...] = packed(layout, *fields)
        spread_rows = pick(coarse_local[:, :chunk], own_hot[...].astype(jnp.bfloat16))
        coarse_rows[...] = spread_rows
        if rides:
            ridden = part(spread_rows, picks[keep.place("to_column"), :])
        else:
            ridden = jnp.zeros((column + PLAIN, lanes), jnp.float32)
        rings[...] = cat([ringed, ridden])

    def begin(
        load, matrix, inverse, basis_in, places, own_table,
        bank, rings, flats, weighted, coarse_rows, picks,
        natural, right, tau, spread, own_hot, basis, load_inside, begun, rest,
    ):
        prepare(
            load, inverse, basis_in, places, own_table, natural, right, tau, weighted, spread, own_hot,
            basis, picks, load_inside, begun,
        )
        start(
            matrix, right, natural, tau, spread, own_hot, basis, picks, bank, rings, flats,
            coarse_rows, rest,
        )

    bank, rings, flats, weighted, coarse_rows, picks = call(
        begin,
        (element_load, local_matrix, dirichlet_inverse, coarse_basis, places, own_table),
        (
            floats(keep.rows["bank"], lanes), floats(count * ring_rows + column + PLAIN, lanes),
            floats(count * (rows - ring_rows), lanes), floats(chunk, rows), floats(chunk, coarse),
            floats(keep.rows["picks"], pick_lanes),
        ),
        scratch=[
            VMEM(shape, jnp.float32)
            for shape in (
                (nodes, lanes), (nodes, lanes + 128), (8, lanes), (rows, coarse), (chunk, coarse),
                (chunk, nodes), (inside, lanes), (inside, lanes), (nodes, lanes),
            )
        ],
    )
    keep.arrays.update(bank=bank, picks=picks)

    def reorder(neumann, places, weighted):
        order, share = places[0:1, :], places[1:2, :]
        across = one_hot_columns(order, nodes)
        surface = one_hot_rows(as_column(order), nodes)
        scaled = pick(surface, pick(neumann[0, 0, 0], across)) * as_column(share) * share
        fill = jnp.zeros((loads_rows - rows - chunk, rows), jnp.float32)
        return stacked(jnp.concatenate([scaled, weighted, fill], axis=0))

    def surface_columns(matrix, places):
        return pick(matrix[0, 0, 0], one_hot_columns(places[0:1, :], nodes))

    def condense(picked, inverse, places, schur, out):
        picked, places = picked[...], places[...]
        surface = one_hot_rows(as_column(places[0:1, :]), nodes)
        within = pick(surface, picked)
        coupling = jnp.concatenate(
            [picked[(i * n + j) * n + 1 : (i * n + j) * n + 1 + deep] for i, j in inner_pairs], axis=0
        )
        out[...] = coupling
        schur[...] = stacked(within - dot(coupling, dot(inverse[0, 0, 0], coupling), (0, 0)))

    def make_columns():
        keep.arrays["columns"] = run(surface_columns, local_matrix, places, flops=FILL)
        return ()

    def make_schur():
        keep.arrays["schur"], keep.arrays["coupling"] = call(
            condense, (keep.arrays.pop("columns"), dirichlet_inverse, places),
            (jax.ShapeDtypeStruct((3 * rows, rows), jnp.bfloat16), floats(inside, rows)), flops=FILL,
        )
        return ()

    def make_scaled():
        keep.arrays["scaled"] = run(reorder, neumann_inverse, places, weighted, flops=FILL)
        return ()

    step = coarse // PIECES

    def invert(first, last):
        for piece in range(first, last):

            def eliminated(matrix, piece=piece):
                return eliminate(matrix, range(piece * step, (piece + 1) * step))

            keep.arrays["coarse"] = run(eliminated, keep.arrays["coarse"], flops=FILL)

    def invert_first():
        if rides:
            invert(0, 1)
        return ()

    def invert_more():
        if rides:
            invert(1, PIECES - 1)
        return ()

    def finish_inverse():
        if rides:
            invert(PIECES - 1, PIECES)
        lifted = lambda spread, inverse: stacked(dot(spread, inverse))
        keep.arrays["lift"] = run(lifted, keep.arrays.pop("spread"), keep.arrays.pop("coarse"))
        return ()

    def other_inverse():
        spread_rows = jnp.broadcast_to(coarse_rows[None], (devices, *coarse_rows.shape))
        gathered = lax.all_to_all(spread_rows, AXES, 0, 0, tiled=True).reshape(-1, coarse)
        ids = jnp.asarray(table[:, :chunk].reshape(1, -1))
        summed = run(lambda ids, rows: pick(one_hot_columns(ids, coarse), rows), ids, gathered)
        factor = jnp.linalg.cholesky(summed)
        eye = jnp.eye(coarse, dtype=jnp.float32)
        return jax.scipy.linalg.cho_solve((factor, True), eye)

    def neumann_step(field, scaled):
        both = product(scaled, field)
        return both[:rows], both[rows : rows + chunk]

    def sent(field, loads, chosen, *extra):
        ringed, flats = packed(layout, field)
        return cat([ringed, part(loads, chosen, *extra)]), flats

    def first(field, *rest):
        pieces, (summed, _, scaled, chosen) = rest[:-4], rest[-4:]
        mapped, loads = neumann_step(field, scaled)
        spread = jnp.concatenate(pieces, axis=1) if len(pieces) > 1 else pieces[0]
        return (spread, summed, *sent(mapped, loads, chosen), field)

    keep.arrays["spread"], keep.arrays["coarse"], rings, flats = assemble(
        layout, count, shares, rings, flats, first, keep, ("scaled", "to_column"),
        ("residual",), make_columns, make_schur, make_scaled,
    )
    if not rides:
        keep.arrays["coarse"] = other_inverse()

    def apply_first(mapped, summed, _, condensed, tau, load, schur, lift):
        field = mapped + product(lift, summed)
        image = product(schur, field)
        energy = tau[:1] + jnp.sum(condensed * field, axis=0, keepdims=True)
        curvature = tau[:1] + jnp.sum(field * image, axis=0, keepdims=True)
        fill = jnp.zeros((6, lanes), jnp.float32)
        sums = jnp.concatenate([energy, curvature, fill], axis=0)
        return (*packed(layout, image, load), field, image, sums)

    rings, flats = assemble(
        layout, 1, shares, rings, flats, apply_first, keep,
        ("condensed", "tau", "load", "schur", "lift"), ("field0", "image0", "totals"), invert_first,
        invert_more, finish_inverse,
    )

    def second(image, load, sums, scaled, chosen):
        mapped, loads = neumann_step(image, scaled)
        return (*sent(mapped, loads, chosen, sums[:2]), image, load)

    rings, flats = assemble(
        layout, 2, None, rings, flats, second, keep,
        ("totals", "scaled", "to_column"), ("image0_sum", "load_sum"),
    )

    def apply_second(mapped, summed, totals, schur, condensed, tau, field0, image0, lift):
        field = mapped + product(lift, summed)
        image = product(schur, field)
        step = totals[:1] / totals[1:2]
        rest = 1.0 - step
        direction = field0 - step * field
        direction_image = image0 - step * image
        energy = rest * rest * tau[:1] + jnp.sum(
            (condensed - step * image0) * direction, axis=0, keepdims=True
        )
        curvature = rest * rest * tau[:1] + jnp.sum(
            direction * direction_image, axis=0, keepdims=True
        )
        cross = rest * tau[:1] + jnp.sum(direction * image0, axis=0, keepdims=True)
        ringed, flats = packed(layout, image)
        fill = jnp.zeros((PLAIN - 3, lanes), jnp.float32)
        return cat([ringed, energy, curvature, cross, fill]), flats, field, totals

    rings, flats = assemble(
        layout, 1, shares, rings, flats, apply_second, keep,
        ("schur", "condensed", "tau", "field0", "image0", "lift"), ("field1", "totals"),
    )

    def put(out, surface, deep_rows, load, factor):
        m, block = n - 1, layout.block
        for i in range(n):
            for s, j in ((0, 0), (1, m)):
                out[i, j, pl.ds(0, m), :] = surface[pl.ds(s * block + i * m, m), :]
                out[i, j, pl.ds(m, 1), :] = surface[pl.ds((s + 2) * block + i * m + m - 1, 1), :]
            for j in range(1, m):
                for s, k in ((2, 0), (3, m)):
                    out[i, j, pl.ds(k, 1), :] = surface[pl.ds(s * block + i * m + j - 1, 1), :]
                if i in (0, m):
                    at = layout.ring_rows + (layout.flat if i else 0) + (j - 1) * deep
                    out[i, j, pl.ds(1, deep), :] = surface[pl.ds(at, deep), :]
                elif deep_rows is None:
                    out[i, j, pl.ds(1, deep), :] = factor * load[i, j, pl.ds(1, deep), :]
                else:
                    at = ((i - 1) * deep + j - 1) * deep
                    out[i, j, pl.ds(1, deep), :] = deep_rows[pl.ds(at, deep), :]

    def solve_inside(bank, coupling, inverse, load, out, inner_load):
        for index, (i, j) in enumerate(inner_pairs):
            inner_load[pl.ds(index * deep, deep), :] = load[i, j, pl.ds(1, deep), :]
        fields = jnp.concatenate([bank[keep.place("field0"), :], bank[keep.place("field1"), :]], axis=1)
        loads = jnp.concatenate([inner_load[...], inner_load[...]], axis=1)
        right = loads - dot(coupling[...], fields)
        out[...] = dot(inverse[0, 0, 0], right)

    def finish_inside():
        (keep.arrays["deep"],) = call(
            solve_inside, (keep.arrays["bank"], keep.arrays["coupling"], dirichlet_inverse, element_load),
            (floats(inside, 2 * lanes),), scratch=[VMEM((inside, lanes), jnp.float32)], flops=FILL,
        )
        return ()

    def leftover(image1, sums, totals, field0, field1, image0, residual, load_sum):
        energy, curvature = totals[:1], totals[1:2]
        step = energy / curvature
        energy_next, curvature_next, cross = sums[:1], sums[1:2], sums[2:3]
        ratio = energy_next / energy
        curvature_next = curvature_next + 2.0 * ratio * cross + ratio * ratio * curvature
        step_next = energy_next / curvature_next
        first = step + step_next * (1.0 + ratio)
        second = -step_next * step
        spill = load_sum - residual
        residual_surface = load_sum - first * (image0 + spill) - second * (image1 + spill)
        fill = jnp.zeros((6, lanes), jnp.float32)
        weights = jnp.concatenate([first, second, fill], axis=0)
        return first * field0 + second * field1, residual_surface, weights

    solution_surface, residual_surface, weights = assemble(
        layout, 1, (0, 0), rings, flats, leftover, keep,
        ("totals", "field0", "field1", "image0_sum", "residual", "load_sum"), (), None,
        finish_inside,
    )

    def place(solution_surface, residual_surface, weights, both, load, one, two, deep_rows):
        first, second = weights[0:1, :], weights[1:2, :]
        deep_rows[...] = first * both[:, :lanes] + second * both[:, lanes:]
        put(one, solution_surface, deep_rows, None, None)
        put(two, residual_surface, None, load, 1.0 - first - second)

    shape = floats(*element_load.shape)
    solution_out, residual_out = call(
        place, (solution_surface, residual_surface, weights, keep.arrays["deep"], element_load),
        (shape, shape), scratch=[VMEM((inside, lanes), jnp.float32)],
    )
    return solution_out, residual_out


def solution(mesh):
    in_specs = (
        P("gx", "gy", "gz", None),
        P("gx", "gy", "gz", None, None),
        P("gx", "gy", "gz", None, None),
        P("gx", "gy", "gz", None, None),
        P("gx", "gy", "gz", None, None),
    )
    out_specs = (P("gx", "gy", "gz", None), P("gx", "gy", "gz", None))
    return jax.shard_map(local, mesh=mesh, in_specs=in_specs, out_specs=out_specs, check_vma=False)
```

```python
import jax
import jax.numpy as jnp
import numpy as np
from jax import lax
from jax.experimental import pallas as pl
from jax.experimental.pallas import tpu as pltpu
from jax.sharding import PartitionSpec as P

AXES = ("gx", "gy", "gz")
HIGHEST = lax.Precision.HIGHEST
PALLAS = True
LIMIT = 24 * 2**20
VMEM = pltpu.VMEM
PIECES = 8
PLAIN = 8
FILL = 10**8


def dot(left, right, contract=(1, 0)):
    dims = (((contract[0],), (contract[1],)), ((), ()))
    return lax.dot_general(
        left, right, dims, precision=HIGHEST, preferred_element_type=jnp.float32
    )


def whole(count):
    return [pl.BlockSpec(memory_space=VMEM)] * count


def call(body, operands, outs, scratch=(), in_hbm=(), flops=10**6, aliases=None):
    places = whole(len(operands))
    for index in in_hbm:
        places[index] = pl.BlockSpec(memory_space=pl.ANY)
    size = sum(4 * np.prod(x.shape) for x in (*operands, *outs))
    return pl.pallas_call(
        body,
        out_shape=[jax.ShapeDtypeStruct(x.shape, x.dtype) for x in outs],
        in_specs=places,
        out_specs=whole(len(outs)),
        scratch_shapes=scratch,
        input_output_aliases=aliases or {},
        compiler_params=pltpu.CompilerParams(vmem_limit_bytes=LIMIT),
        cost_estimate=pl.CostEstimate(flops=flops, bytes_accessed=int(size), transcendentals=0),
    )(*operands)


def run(function, *operands, flops=10**6, after=(), keep=None, use=(), store=()):
    arrays = {} if keep is None else keep.arrays
    names = list(arrays)
    used = [keep.read(arrays, name) for name in use]
    shapes = jax.eval_shape(function, *operands, *used)
    single = not isinstance(shapes, tuple)
    outs = (shapes,) if single else shapes
    outs = outs[: len(outs) - len(store)]
    count = len(operands)
    base = count + len(after)
    first_out = base + len(names)

    def body(*refs):
        kept = dict(zip(names, refs[base:first_out]))
        kept_out = dict(zip(names, refs[first_out + len(outs) :]))
        values = [ref[...] for ref in refs[:count]] + [keep.read(kept, name) for name in use]
        results = function(*values)
        results = (results,) if single else results
        for ref, result in zip(refs[first_out:], results[: len(outs)]):
            ref[...] = result
        for name, result in zip(store, results[len(outs) :]):
            bank, start, _ = keep.slots[name]
            kept_out[bank][pl.ds(start, result.shape[0]), :] = result

    held = [arrays[name] for name in names]
    aliases = {base + index: len(outs) + index for index in range(len(names))}
    results = call(
        body, (*operands, *after, *held), (*outs, *held), in_hbm=range(count, base), flops=flops,
        aliases=aliases,
    )
    arrays.update(zip(names, results[len(outs) :]))
    results = results[: len(outs)]
    return results[0] if single and results else tuple(results)


class Keep:
    def __init__(self):
        self.arrays, self.slots, self.rows = {}, {}, {}

    def plan(self, bank, sizes):
        self.rows[bank] = 0
        for name, size in sizes:
            self.slots[name] = (bank, self.rows[bank], size)
            self.rows[bank] += -(-size // 8) * 8

    def place(self, name):
        _, start, size = self.slots[name]
        return pl.ds(start, size)

    def read(self, arrays, name):
        name, wanted = name if isinstance(name, tuple) else (name, None)
        if name in self.slots:
            bank, start, size = self.slots[name]
            return arrays[bank][start : start + (wanted or size), :]
        return arrays[name][...]


def floats(*shape):
    return jax.ShapeDtypeStruct(shape, jnp.float32)


class Layout:
    def __init__(self, n):
        m = n - 1
        self.n, self.m = n, m
        self.block = n * m
        self.ring_rows = 4 * self.block
        flat = (n - 2) ** 2
        self.flat = -(-flat // 8) * 8
        self.rows = self.ring_rows + 2 * self.flat
        self.y_rows = self.block + -(-n // 8) * 8
        self.x_rows = 4 * m + self.flat
        at = lambda i, j, k: (i * n + j) * n + k
        inner = range(1, m)
        order = [at(i, j, k) for j in (0, m) for i in range(n) for k in range(m)]
        for j, k in ((0, 0), (m, m)):
            for i in range(n):
                order += [at(i, x, k) for x in inner] + [at(i, j, m)]
        for i in (0, m):
            order += [at(i, j, k) for j in inner for k in inner]
            order += [-1] * (self.flat - flat)
        self.order = np.array(order, np.int32)
        self.inner = np.array([at(i, j, k) for i in inner for j in inner for k in inner], np.int32)
        share = np.zeros((self.rows, 1), np.float32)
        for row, node in enumerate(order):
            if node >= 0:
                place = (node // (n * n), node // n % n, node % n)
                share[row] = 0.5 ** sum(x in (0, m) for x in place)
        self.share = share

    def blocks(self, ring):
        return [ring[s * self.block : (s + 1) * self.block] for s in range(4)]

    def row_in_tile(self, block):
        return lax.broadcasted_iota(jnp.int32, block.shape, 0) % self.m

    def fold_z(self, ring, below, above):
        first, last, low, high = self.blocks(ring)
        below, above = self.blocks(below), self.blocks(above)
        row = self.row_in_tile(first)
        start, end = row == 0, row == self.m - 1
        back = lambda x: roll_rows(x, x.shape[0] - (self.m - 1))
        ahead = lambda x: roll_rows(x, self.m - 1)
        zero = jnp.zeros_like(first)
        first = first + jnp.where(start, back(below[2]), zero)
        last = last + jnp.where(start, back(below[3]), zero)
        low = low + jnp.where(end, ahead(above[0]), below[3])
        high = high + jnp.where(end, ahead(above[1]), above[2])
        return jnp.concatenate([first, last, low, high], axis=0)

    def side(self, block, corners):
        lanes = block.shape[1]
        rows = corners.reshape(self.n, self.m, lanes)[:, self.m - 1, :]
        fill = jnp.zeros((self.y_rows - self.block - self.n, lanes), block.dtype)
        return jnp.concatenate([block, rows, fill], axis=0)

    def sides_y(self, ring):
        first, last, low, high = self.blocks(ring)
        return self.side(first, low), self.side(last, high)

    def fold_y(self, ring, below, above):
        first, last, low, high = self.blocks(ring)
        lanes = ring.shape[1]
        end = self.row_in_tile(first) == self.m - 1

        def ends(message):
            rows = message[self.block : self.block + self.n].reshape(self.n, 1, lanes)
            wide = jnp.broadcast_to(rows, (self.n, self.m, lanes)).reshape(self.block, lanes)
            return jnp.where(end, wide, jnp.zeros_like(wide))

        first = first + below[: self.block]
        low = low + ends(below)
        last = last + above[: self.block]
        high = high + ends(above)
        return jnp.concatenate([first, last, low, high], axis=0)

    def sides_x(self, ring, flat):
        m, block = self.m, self.block
        low = [ring[s * block : s * block + m] for s in range(4)] + [flat[: self.flat]]
        high = [ring[(s + 1) * block - m : (s + 1) * block] for s in range(4)] + [flat[self.flat :]]
        return jnp.concatenate(low, axis=0), jnp.concatenate(high, axis=0)

    def fold_x(self, ring, flat, below, above):
        m, block = self.m, self.block
        parts = []
        for s in range(4):
            parts += [
                ring[s * block : s * block + m] + below[s * m : (s + 1) * m],
                ring[s * block + m : (s + 1) * block - m],
                ring[(s + 1) * block - m : (s + 1) * block] + above[s * m : (s + 1) * m],
            ]
        parts += [flat[: self.flat] + below[4 * m :], flat[self.flat :] + above[4 * m :]]
        return jnp.concatenate(parts, axis=0)


def roll_rows(value, shift):
    if PALLAS:
        return pltpu.roll(value, shift, 0)
    return jnp.roll(value, shift, axis=0)


def shifted(value, axis, step):
    size = lax.axis_size(axis)
    return lax.ppermute(value, axis, [(i, (i + step) % size) for i in range(size)])


def both_ways(low, high, axis):
    return shifted(high, axis, 1), shifted(low, axis, -1)


def cat(parts):
    return parts[0] if len(parts) == 1 else jnp.concatenate(parts, axis=0)


def packed(layout, *fields):
    rings, rows = layout.ring_rows, layout.rows
    return cat([f[:rings] for f in fields]), cat([f[rings:rows] for f in fields])


def steps_of(axis):
    size = lax.axis_size(axis)
    return [1] if size == 2 else [1, size - 1, *range(2, size - 1)]


def assemble(
    layout, count, shares, rings, flats, function, keep, use=(), store=(), beside_z=None, beside_y=None,
    beside_x=None,
):
    ring_rows, flat_rows = layout.ring_rows, layout.rows - layout.ring_rows
    split = lambda value, size: [value[i * size : (i + 1) * size] for i in range(count)]
    column, slab = shares or (0, 0)
    far_steps = lambda axis: steps_of(axis)[2:] if shares else []
    picked = lambda name: (name,) if column else ()

    steps = [*steps_of("gz")[:2], *far_steps("gz")]
    sums = rings[count * ring_rows :] if len(steps) > 2 else None
    others = [shifted(rings, "gz", step) for step in steps[:2]]
    others += [shifted(sums, "gz", step) for step in steps[2:]]
    ties = beside_z() if beside_z else ()
    near = len(steps_of("gz")[:2])

    def after_z(rings, flats, *others):
        done, low, high = [], [], []
        parts = [split(value, ring_rows) for value in (rings, others[0], others[near - 1])]
        for ring, below, above in zip(*parts):
            if near == 1:
                above = below
            ring = layout.fold_z(ring, below, above)
            sides = layout.sides_y(ring)
            done.append(ring)
            low.append(sides[0])
            high.append(sides[1])
        if not shares:
            return cat(low), cat(high), cat([*done, flats])
        own = rings[count * ring_rows :]
        for index, other in enumerate(others):
            own = own + (other[count * ring_rows :] if index < near else other)
        return cat([*low, own]), cat([*high, own]), own, cat([*done, flats])

    work = ("work", count * layout.rows)
    low, high, *own = run(after_z, rings, flats, *others, after=ties, keep=keep, store=("work",))
    far = [shifted(own[0], "gy", step) for step in far_steps("gy")]
    below, above = both_ways(low, high, "gy")
    ties = beside_y() if beside_y else ()

    def all_parts(own, below, above, far, edge, axis):
        parts = [own, below[edge:]]
        return parts + ([above[edge:]] if len(steps_of(axis)) > 1 else []) + list(far)

    def merged(chosen, parts, size):
        plain = sum(part[size:] for part in parts)
        if not size:
            return (plain,)
        wide = cat([part[:size] for part in parts])
        return pick(chosen[0][:, : wide.shape[0]].astype(jnp.bfloat16), wide), plain

    def after_y(below, above, *rest):
        own, rest = rest[: len(own_y)], rest[len(own_y) :]
        far, both, chosen = rest[: len(far_y)], rest[len(far_y)], rest[len(far_y) + 1 :]
        done, low, high = [], [], []
        rings, flats = both[: count * ring_rows], both[count * ring_rows :]
        edge = count * layout.y_rows
        parts = (
            split(rings, ring_rows), split(flats, flat_rows), split(below[:edge], layout.y_rows),
            split(above[:edge], layout.y_rows),
        )
        for ring, flat, first, last in zip(*parts):
            ring = layout.fold_y(ring, first, last)
            sides = layout.sides_x(ring, flat)
            done.append(ring)
            low.append(sides[0])
            high.append(sides[1])
        if not shares:
            return cat(low), cat(high), cat([*done, flats])
        own = cat(merged(chosen, all_parts(own[0], below, above, far, edge, "gy"), column))
        return cat([*low, own]), cat([*high, own]), own, cat([*done, flats])

    own_y, far_y = own, far
    low, high, *own = run(
        after_y, below, above, *own, *far, after=ties, keep=keep, use=(work, *picked("to_slab")),
        store=("work",),
    )
    far = [shifted(own[0], "gx", step) for step in far_steps("gx")]
    below, above = both_ways(low, high, "gx")
    ties = beside_x() if beside_x else ()

    def after_x(below, above, *rest):
        own_x, rest = rest[: len(own)], rest[len(own) :]
        far_x, both, rest = rest[: len(far)], rest[len(far)], rest[len(far) + 1 :]
        chosen, rest = (rest[:1], rest[1:]) if column else ((), rest)
        rings, flats = both[: count * ring_rows], both[count * ring_rows :]
        edge = count * layout.x_rows
        parts = (
            split(rings, ring_rows), split(flats, flat_rows), split(below[:edge], layout.x_rows),
            split(above[:edge], layout.x_rows),
        )
        sums = ()
        if shares:
            sums = merged(chosen, all_parts(own_x[0], below, above, far_x, edge, "gx"), slab)
        return function(*[layout.fold_x(*values) for values in zip(*parts)], *sums, *rest)

    return run(
        after_x, below, above, *own, *far, after=ties, keep=keep,
        use=(work, *picked("to_all"), *use), store=store,
    )


def parts_of(value):
    high = value.astype(jnp.bfloat16)
    rest = value - high.astype(jnp.float32)
    middle = rest.astype(jnp.bfloat16)
    low = (rest - middle.astype(jnp.float32)).astype(jnp.bfloat16)
    return high, middle, low


def pick(left, right, contract=(1, 0)):
    dims = (((contract[0],), (contract[1],)), ((), ()))
    if left.dtype == jnp.bfloat16:
        pairs = [(left, part) for part in parts_of(right)]
    else:
        pairs = [(part, right) for part in parts_of(left)]
    terms = [lax.dot_general(a, b, dims, preferred_element_type=jnp.float32) for a, b in pairs]
    return terms[0] + terms[1] + terms[2]


def stacked(value):
    return jnp.concatenate(parts_of(value), axis=0)


def product(stack, right):
    rows, lanes = stack.shape[0] // 3, right.shape[1]
    high, middle, low = parts_of(right)
    times = lambda a, b: jnp.dot(a, b, preferred_element_type=jnp.float32)
    wide = times(stack[: 2 * rows], jnp.concatenate([high, middle], axis=1))
    small = wide[rows:, lanes:] + times(stack[:rows], low) + times(stack[2 * rows :], high)
    return wide[:rows, :lanes] + (wide[:rows, lanes:] + wide[rows:, :lanes] + small)


def runs_of(places):
    found, at = [], 0
    while at < len(places):
        if places[at] < 0:
            at += 1
            continue
        size, stride = 1, 1
        if at + 1 < len(places) and places[at + 1] > places[at]:
            stride = int(places[at + 1] - places[at])
            while at + size < len(places) and places[at + size] - places[at + size - 1] == stride:
                size += 1
            if size == 2 and stride > 1:
                size = 1
        found.append((at, int(places[at]), size, stride if size > 1 else 1))
        at += size
    return found


def one_hot_rows(column, count):
    lanes = lax.broadcasted_iota(jnp.int32, (column.shape[0], count), 1).astype(jnp.float32)
    return jnp.where(lanes == column, 1.0, 0.0).astype(jnp.bfloat16)


def one_hot_columns(row, count):
    places = lax.broadcasted_iota(jnp.int32, (count, row.shape[1]), 0).astype(jnp.float32)
    return jnp.where(places == row, 1.0, 0.0).astype(jnp.bfloat16)


def as_column(row):
    return jnp.broadcast_to(row, (8, row.shape[1])).T[:, :1]


def up(value, step):
    return -(-value // step) * step


def coarse_tables(counts, constraints):
    x, y, z = counts
    total = x * y * z

    def number(kind, i, j, k):
        return kind * total + (i % x * y + j % y) * z + k % z

    def own(a, b, c):
        two = (0, 1)
        listed = [number(0, a + i, b + j, c + k) for i in two for j in two for k in two]
        listed += [number(1, a, b + j, c + k) for j in two for k in two]
        listed += [number(2, a + i, b, c + k) for i in two for k in two]
        return listed + [number(3, a + i, b + j, c) for i in two for j in two]

    def unique(lists, pad):
        listed = sorted(set(sum(lists, [])))
        return listed + [pad] * (up(len(listed), 8) - len(listed))

    column = lambda a, b, pad: unique([own(a, b, c) for c in range(z)], pad)
    slab = lambda a, pad: unique([own(a, b, c) for b in range(y) for c in range(z)], pad)
    back_y = [0] + steps_of("gy")
    back_x = [0] + steps_of("gx")
    rows = []
    for a in range(x):
        for b in range(y):
            for c in range(z):
                first = own(a, b, c)
                rows.append([
                    first + [-1] * (constraints - len(first)), column(a, b, -2),
                    sum([column(a, (b - s) % y, -3) for s in back_y], []), slab(a, -4),
                    sum([slab((a - s) % x, -5) for s in back_x], []),
                ])
    starts, width = [], 0
    for listed in rows[0]:
        starts.append(width)
        width += up(len(listed), 128)
    table = np.full((total, width), -9, np.float32)
    for row, lists in zip(table, rows):
        for start, listed in zip(starts, lists):
            row[start : start + len(listed)] = listed
    sizes = [len(listed) for listed in rows[0]]
    return table, starts, sizes


def eliminate(matrix, pivots):
    count = matrix.shape[0]
    rows = lax.broadcasted_iota(jnp.int32, (8, count), 0)
    lanes = lax.broadcasted_iota(jnp.int32, (1, count), 1)
    for k in pivots[::2]:
        m, tile = k + 1, k // 8 * 8
        spread = lambda lane: jnp.take_along_axis(
            matrix, jnp.full(matrix.shape, lane, jnp.int32), axis=1
        )
        column0, column1 = spread(k), spread(m)
        a, b, d = column0[k:m], column1[k:m], column1[m : m + 1]
        scale = 1.0 / (a * d - b * b)
        here = (lanes == k) | (lanes == m)
        row0 = jnp.where(here, jnp.where(lanes == k, 1.0, 0.0), matrix[k:m, :])
        row1 = jnp.where(here, jnp.where(lanes == m, 1.0, 0.0), matrix[m : m + 1, :])
        new0 = (d * row0 - b * row1) * scale
        new1 = (a * row1 - b * row0) * scale
        matrix = jnp.where(here, 0.0, matrix) - column0 * new0 - column1 * new1
        own = jnp.where(rows == k - tile, new0, matrix[tile : tile + 8])
        own = jnp.where(rows == m - tile, new1, own)
        parts = [matrix[:tile], own, matrix[tile + 8 :]]
        matrix = jnp.concatenate([part for part in parts if part.shape[0]], axis=0)
    return matrix


def local(element_load, local_matrix, dirichlet_inverse, neumann_inverse, coarse_basis):
    n = element_load.shape[0]
    lanes = element_load.shape[3]
    nodes = n**3
    layout = Layout(n)
    inside = (n - 2) ** 3
    primal = coarse_basis.shape[3]
    counts = [lax.axis_size(axis) for axis in AXES]
    devices = counts[0] * counts[1] * counts[2]
    coarse = 4 * devices
    chunk = -(-primal // 8) * 8
    rows = layout.rows
    table, starts, sizes = coarse_tables(counts, chunk)
    shares = column, slab = sizes[1], sizes[3]
    rides = coarse == lanes
    own_table = jnp.asarray(table)
    places = np.stack([layout.order.astype(np.float32), layout.share[:, 0]])
    places = jnp.asarray(np.pad(places, ((0, 6), (0, 0))))
    pairs = [(i, j) for i in range(n) for j in range(n)]
    inner_pairs = [(i, j) for i in range(1, n - 1) for j in range(1, n - 1)]
    deep = n - 2


    count = 1 + -(-coarse // lanes)
    ring_rows = layout.ring_rows
    names = ("condensed", "load", "residual", "field0", "image0", "image0_sum", "load_sum", "field1")
    keep = Keep()
    keep.plan(
        "bank",
        [("tau", 8), ("totals", 8), ("work", max(count, 2) * rows)] + [(name, rows) for name in names],
    )
    keep.plan("picks", [("to_column", column), ("to_slab", slab), ("to_all", coarse)])
    pick_lanes = up(max(sizes), 128)
    loads_rows = up(rows + chunk, 16)

    def prepare(
        load, inverse, basis_in, places, own_table,
        natural, right, tau, weighted, spread, own_hot, basis, picks, load_inside, begun,
    ):
        order = places[0:1, :]
        across = one_hot_columns(order, nodes)
        for i, j in pairs:
            natural[pl.ds((i * n + j) * n, n), :] = load[i, j]
        for index, (i, j) in enumerate(inner_pairs):
            load_inside[pl.ds(index * deep, deep), :] = load[i, j, pl.ds(1, deep), :]
        begun[...] = dot(inverse[0, 0, 0], load_inside[...])
        tau[...] = jnp.broadcast_to(
            jnp.sum(load_inside[...] * begun[...], axis=0, keepdims=True), (8, lanes)
        )
        right[:, pl.ds(0, lanes)] = jnp.zeros((nodes, lanes), jnp.float32)
        for index, (i, j) in enumerate(inner_pairs):
            right[pl.ds((i * n + j) * n + 1, deep), pl.ds(0, lanes)] = begun[
                pl.ds(index * deep, deep), :
            ]
        basis[...] = jnp.concatenate(
            [basis_in[0, 0, 0], jnp.zeros((chunk - primal, nodes), jnp.float32)], axis=0
        )
        right[:, pl.ds(lanes, 128)] = jnp.concatenate(
            [basis[...], jnp.zeros((128 - chunk, nodes), jnp.float32)], axis=0
        ).T
        weighted[...] = pick(basis[...], across) * places[1:2, :]
        me = own_table[pl.ds(lax.axis_index(AXES), 1), :]
        lists = [me[:, s : s + up(size, 128)] for s, size in zip(starts, sizes)]
        own = one_hot_rows(as_column(lists[0])[:chunk], coarse)
        own_hot[...] = own.astype(jnp.float32)
        spread[...] = pick(weighted[...], own, (0, 0))

        def match(name, targets, sources, size):
            found = jnp.where(targets == sources, 1.0, 0.0)
            lane = lax.broadcasted_iota(jnp.int32, found.shape, 1)
            picks[keep.place(name), pl.ds(0, found.shape[1])] = jnp.where(lane < size, found, 0.0)

        match("to_column", as_column(lists[1])[:column], lists[0], chunk)
        match("to_slab", as_column(lists[3])[:slab], lists[2], sizes[2])
        every = lax.broadcasted_iota(jnp.int32, (coarse, 1), 0).astype(jnp.float32)
        match("to_all", every, lists[4], sizes[4])

    def part(loads, chosen, *extra):
        mapped = pick(chosen[:, :chunk].astype(jnp.bfloat16), loads)
        fill = jnp.zeros((PLAIN - sum(rows.shape[0] for rows in extra), lanes), jnp.float32)
        return cat([mapped, *extra, fill])

    moves = runs_of(list(layout.order))
    empty = runs_of([row if node < 0 else -1 for row, node in enumerate(layout.order)])

    def start(
        matrix, right, natural, tau, spread, own_hot, basis, picks,
        bank, rings, flats, coarse_rows, rest,
    ):
        images = dot(matrix[0, 0, 0], right[...])
        coarse_local = dot(basis[...], images[:, lanes:])
        rest[...] = natural[...] - images[:, :lanes]
        bank[keep.place("tau"), :] = tau[...]
        for name, source in (("load", natural), ("condensed", rest)):
            first = keep.slots[name][1]
            for _, row, size, _ in empty:
                bank[pl.ds(first + row, size), :] = jnp.zeros((size, lanes), jnp.float32)
            for at, row, size, stride in moves:
                bank[pl.ds(first + at, size), :] = source[pl.ds(row, size, stride), :]
        fields = [bank[keep.place("condensed"), :]]
        fields += [spread[:, s : s + lanes] for s in range(0, coarse, lanes)]
        ringed, flats[...] = packed(layout, *fields)
        spread_rows = pick(coarse_local[:, :chunk], own_hot[...].astype(jnp.bfloat16))
        coarse_rows[...] = spread_rows
        if rides:
            ridden = part(spread_rows, picks[keep.place("to_column"), :])
        else:
            ridden = jnp.zeros((column + PLAIN, lanes), jnp.float32)
        rings[...] = cat([ringed, ridden])

    def begin(
        load, matrix, inverse, basis_in, places, own_table,
        bank, rings, flats, weighted, coarse_rows, picks,
        natural, right, tau, spread, own_hot, basis, load_inside, begun, rest,
    ):
        prepare(
            load, inverse, basis_in, places, own_table, natural, right, tau, weighted, spread, own_hot,
            basis, picks, load_inside, begun,
        )
        start(
            matrix, right, natural, tau, spread, own_hot, basis, picks, bank, rings, flats,
            coarse_rows, rest,
        )

    bank, rings, flats, weighted, coarse_rows, picks = call(
        begin,
        (element_load, local_matrix, dirichlet_inverse, coarse_basis, places, own_table),
        (
            floats(keep.rows["bank"], lanes), floats(count * ring_rows + column + PLAIN, lanes),
            floats(count * (rows - ring_rows), lanes), floats(chunk, rows), floats(chunk, coarse),
            floats(keep.rows["picks"], pick_lanes),
        ),
        scratch=[
            VMEM(shape, jnp.float32)
            for shape in (
                (nodes, lanes), (nodes, lanes + 128), (8, lanes), (rows, coarse), (chunk, coarse),
                (chunk, nodes), (inside, lanes), (inside, lanes), (nodes, lanes),
            )
        ],
    )
    keep.arrays.update(bank=bank, picks=picks)

    def reorder(neumann, places, weighted):
        order, share = places[0:1, :], places[1:2, :]
        across = one_hot_columns(order, nodes)
        surface = one_hot_rows(as_column(order), nodes)
        scaled = pick(surface, pick(neumann[0, 0, 0], across)) * as_column(share) * share
        fill = jnp.zeros((loads_rows - rows - chunk, rows), jnp.float32)
        return stacked(jnp.concatenate([scaled, weighted, fill], axis=0))

    def surface_columns(matrix, places):
        return pick(matrix[0, 0, 0], one_hot_columns(places[0:1, :], nodes))

    def condense(picked, inverse, places, schur, out):
        picked, places = picked[...], places[...]
        surface = one_hot_rows(as_column(places[0:1, :]), nodes)
        within = pick(surface, picked)
        coupling = jnp.concatenate(
            [picked[(i * n + j) * n + 1 : (i * n + j) * n + 1 + deep] for i, j in inner_pairs], axis=0
        )
        out[...] = coupling
        schur[...] = stacked(within - dot(coupling, dot(inverse[0, 0, 0], coupling), (0, 0)))

    def make_columns():
        keep.arrays["columns"] = run(surface_columns, local_matrix, places, flops=FILL)
        return ()

    def make_schur():
        keep.arrays["schur"], keep.arrays["coupling"] = call(
            condense, (keep.arrays.pop("columns"), dirichlet_inverse, places),
            (jax.ShapeDtypeStruct((3 * rows, rows), jnp.bfloat16), floats(inside, rows)), flops=FILL,
        )
        return ()

    def make_scaled():
        keep.arrays["scaled"] = run(reorder, neumann_inverse, places, weighted, flops=FILL)
        return ()

    step = coarse // PIECES

    def invert(first, last):
        for piece in range(first, last):

            def eliminated(matrix, piece=piece):
                return eliminate(matrix, range(piece * step, (piece + 1) * step))

            keep.arrays["coarse"] = run(eliminated, keep.arrays["coarse"], flops=FILL)

    def invert_first():
        if rides:
            invert(0, 1)
        return ()

    def invert_more():
        if rides:
            invert(1, PIECES - 2)
        return ()

    def finish_inverse():
        if rides:
            invert(PIECES - 2, PIECES)
        lifted = lambda spread, inverse: stacked(dot(spread, inverse))
        keep.arrays["lift"] = run(lifted, keep.arrays.pop("spread"), keep.arrays.pop("coarse"))
        return ()

    def other_inverse():
        spread_rows = jnp.broadcast_to(coarse_rows[None], (devices, *coarse_rows.shape))
        gathered = lax.all_to_all(spread_rows, AXES, 0, 0, tiled=True).reshape(-1, coarse)
        ids = jnp.asarray(table[:, :chunk].reshape(1, -1))
        summed = run(lambda ids, rows: pick(one_hot_columns(ids, coarse), rows), ids, gathered)
        factor = jnp.linalg.cholesky(summed)
        eye = jnp.eye(coarse, dtype=jnp.float32)
        return jax.scipy.linalg.cho_solve((factor, True), eye)

    def neumann_step(field, scaled):
        both = product(scaled, field)
        return both[:rows], both[rows : rows + chunk]

    def sent(field, loads, chosen, *extra):
        ringed, flats = packed(layout, field)
        return cat([ringed, part(loads, chosen, *extra)]), flats

    def first(field, *rest):
        pieces, (summed, _, scaled, chosen) = rest[:-4], rest[-4:]
        mapped, loads = neumann_step(field, scaled)
        spread = jnp.concatenate(pieces, axis=1) if len(pieces) > 1 else pieces[0]
        return (spread, summed, *sent(mapped, loads, chosen), field)

    keep.arrays["spread"], keep.arrays["coarse"], rings, flats = assemble(
        layout, count, shares, rings, flats, first, keep, ("scaled", "to_column"),
        ("residual",), make_columns, make_schur, make_scaled,
    )
    if not rides:
        keep.arrays["coarse"] = other_inverse()

    def apply_first(mapped, summed, _, condensed, tau, load, schur, lift):
        field = mapped + product(lift, summed)
        image = product(schur, field)
        energy = tau[:1] + jnp.sum(condensed * field, axis=0, keepdims=True)
        curvature = tau[:1] + jnp.sum(field * image, axis=0, keepdims=True)
        fill = jnp.zeros((6, lanes), jnp.float32)
        sums = jnp.concatenate([energy, curvature, fill], axis=0)
        return (*packed(layout, image, load), field, image, sums)

    rings, flats = assemble(
        layout, 1, shares, rings, flats, apply_first, keep,
        ("condensed", "tau", "load", "schur", "lift"), ("field0", "image0", "totals"), invert_first,
        invert_more, finish_inverse,
    )

    def second(image, load, sums, scaled, chosen):
        mapped, loads = neumann_step(image, scaled)
        return (*sent(mapped, loads, chosen, sums[:2]), image, load)

    rings, flats = assemble(
        layout, 2, None, rings, flats, second, keep,
        ("totals", "scaled", "to_column"), ("image0_sum", "load_sum"),
    )

    def apply_second(mapped, summed, totals, schur, condensed, tau, field0, image0, lift):
        field = mapped + product(lift, summed)
        image = product(schur, field)
        step = totals[:1] / totals[1:2]
        rest = 1.0 - step
        direction = field0 - step * field
        direction_image = image0 - step * image
        energy = rest * rest * tau[:1] + jnp.sum(
            (condensed - step * image0) * direction, axis=0, keepdims=True
        )
        curvature = rest * rest * tau[:1] + jnp.sum(
            direction * direction_image, axis=0, keepdims=True
        )
        cross = rest * tau[:1] + jnp.sum(direction * image0, axis=0, keepdims=True)
        ringed, flats = packed(layout, image)
        fill = jnp.zeros((PLAIN - 3, lanes), jnp.float32)
        return cat([ringed, energy, curvature, cross, fill]), flats, field, totals

    rings, flats = assemble(
        layout, 1, shares, rings, flats, apply_second, keep,
        ("schur", "condensed", "tau", "field0", "image0", "lift"), ("field1", "totals"),
    )

    def put(out, surface, deep_rows, load, factor):
        m, block = n - 1, layout.block
        for i in range(n):
            for s, j in ((0, 0), (1, m)):
                out[i, j, pl.ds(0, m), :] = surface[pl.ds(s * block + i * m, m), :]
                out[i, j, pl.ds(m, 1), :] = surface[pl.ds((s + 2) * block + i * m + m - 1, 1), :]
            for j in range(1, m):
                for s, k in ((2, 0), (3, m)):
                    out[i, j, pl.ds(k, 1), :] = surface[pl.ds(s * block + i * m + j - 1, 1), :]
                if i in (0, m):
                    at = layout.ring_rows + (layout.flat if i else 0) + (j - 1) * deep
                    out[i, j, pl.ds(1, deep), :] = surface[pl.ds(at, deep), :]
                elif deep_rows is None:
                    out[i, j, pl.ds(1, deep), :] = factor * load[i, j, pl.ds(1, deep), :]
                else:
                    at = ((i - 1) * deep + j - 1) * deep
                    out[i, j, pl.ds(1, deep), :] = deep_rows[pl.ds(at, deep), :]

    def solve_inside(bank, coupling, inverse, load, out, inner_load):
        for index, (i, j) in enumerate(inner_pairs):
            inner_load[pl.ds(index * deep, deep), :] = load[i, j, pl.ds(1, deep), :]
        fields = jnp.concatenate([bank[keep.place("field0"), :], bank[keep.place("field1"), :]], axis=1)
        loads = jnp.concatenate([inner_load[...], inner_load[...]], axis=1)
        right = loads - dot(coupling[...], fields)
        out[...] = dot(inverse[0, 0, 0], right)

    def finish_inside():
        (keep.arrays["deep"],) = call(
            solve_inside, (keep.arrays["bank"], keep.arrays["coupling"], dirichlet_inverse, element_load),
            (floats(inside, 2 * lanes),), scratch=[VMEM((inside, lanes), jnp.float32)], flops=FILL,
        )
        return ()

    def leftover(image1, sums, totals, field0, field1, image0, residual, load_sum):
        energy, curvature = totals[:1], totals[1:2]
        step = energy / curvature
        energy_next, curvature_next, cross = sums[:1], sums[1:2], sums[2:3]
        ratio = energy_next / energy
        curvature_next = curvature_next + 2.0 * ratio * cross + ratio * ratio * curvature
        step_next = energy_next / curvature_next
        first = step + step_next * (1.0 + ratio)
        second = -step_next * step
        spill = load_sum - residual
        residual_surface = load_sum - first * (image0 + spill) - second * (image1 + spill)
        fill = jnp.zeros((6, lanes), jnp.float32)
        weights = jnp.concatenate([first, second, fill], axis=0)
        return first * field0 + second * field1, residual_surface, weights

    solution_surface, residual_surface, weights = assemble(
        layout, 1, (0, 0), rings, flats, leftover, keep,
        ("totals", "field0", "field1", "image0_sum", "residual", "load_sum"), (), None,
        finish_inside,
    )

    def place(solution_surface, residual_surface, weights, both, load, one, two, deep_rows):
        first, second = weights[0:1, :], weights[1:2, :]
        deep_rows[...] = first * both[:, :lanes] + second * both[:, lanes:]
        put(one, solution_surface, deep_rows, None, None)
        put(two, residual_surface, None, load, 1.0 - first - second)

    shape = floats(*element_load.shape)
    solution_out, residual_out = call(
        place, (solution_surface, residual_surface, weights, keep.arrays["deep"], element_load),
        (shape, shape), scratch=[VMEM((inside, lanes), jnp.float32)],
    )
    return solution_out, residual_out


def solution(mesh):
    in_specs = (
        P("gx", "gy", "gz", None),
        P("gx", "gy", "gz", None, None),
        P("gx", "gy", "gz", None, None),
        P("gx", "gy", "gz", None, None),
        P("gx", "gy", "gz", None, None),
    )
    out_specs = (P("gx", "gy", "gz", None), P("gx", "gy", "gz", None))
    return jax.shard_map(local, mesh=mesh, in_specs=in_specs, out_specs=out_specs, check_vma=False)
```
